32 devices in a mesh: dp: 2 (over x), tp: 4 (over z), cp: 4 (over y, core).
Axes of the slice: x: 2, y: 2, z: 4, core: 2. Of those that a mesh axis runs over, the one named last changes fastest.
Arguments:
- x: bfloat16 [1024, 3072], P(('dp', 'cp', 'tp')), parts along dimension 0
- pos: int32 [1024], P(('dp', 'cp', 'tp')), parts along dimension 0
- g1: bfloat16 [3072], replicated
- g2: bfloat16 [3072], replicated
- wq: bfloat16 [3072, 3072], P(None, 'tp')
- wk: bfloat16 [3072, 1024], P(None, 'tp')
- wv: bfloat16 [3072, 1024], P(None, 'tp')
- wo: bfloat16 [3072, 3072], P('tp')
- w1: bfloat16 [3072, 8192], P(None, 'tp')
- w3: bfloat16 [3072, 8192], P(None, 'tp')
- w2: bfloat16 [8192, 3072], P('tp')
Outputs:
- output: bfloat16 [1024, 3072], P(('dp', 'cp', 'tp')), parts along dimension 0
There are 2 independent parts. The reference program is written for one: setup_inputs(seed, part) draws one part's arguments, and reference() takes and returns one part's arrays. A program takes and returns all parts, laid end to end along the dimension named above; an argument that names none is the same for every part.
All inputs are finite; a program needn't handle non-finite values.
Results may differ from the reference program's by a relative error of at most 0.0106727.
Values are sent between devices in bfloat16 or wider.
A program may use at most 1 GiB of HBM per device.

```python
import math
import jax
import jax.numpy as jnp
from jax import lax

T = 512
D = 3072
HQ = 24
HKV = 8
DH = 128
F = 8192
NDEV = 16
QB = 64
PIECE = T // (2 * NDEV)
GRP = HQ // HKV
EPS = 1e-5
THETA = 500000.0


def setup_inputs(seed: int = 0, part: int = 0) -> dict:
    kpart = jax.random.fold_in(jax.random.key(seed), part)
    kx, kgap, kstart = jax.random.split(kpart, 3)
    kw = jax.random.split(jax.random.key(seed + 1), 9)
    x = jax.random.normal(kx, (T, D), jnp.float32).astype(jnp.bfloat16)
    gaps = jax.random.randint(kgap, (T,), 1, 4)
    start = jax.random.randint(kstart, (), 0, T)
    seqpos = start + jnp.cumsum(gaps) - gaps[0]
    rows = jnp.arange(T)
    dev = rows // (2 * PIECE)
    off = rows % (2 * PIECE)
    piece = jnp.where(off < PIECE, dev, 2 * NDEV - 1 - dev)
    pos = seqpos[piece * PIECE + off % PIECE].astype(jnp.int32)
    qk = math.sqrt(math.sqrt(math.log(T / 16.0)))

    def nrm(k, shape, scl):
        return (jax.random.normal(k, shape, jnp.float32) * scl).astype(jnp.bfloat16)

    g1 = (1.0 + 0.3 * jax.random.normal(kw[0], (D,), jnp.float32)).astype(jnp.bfloat16)
    g2 = (1.0 + 0.3 * jax.random.normal(kw[1], (D,), jnp.float32)).astype(jnp.bfloat16)
    wq = nrm(kw[2], (D, HQ * DH), qk / math.sqrt(D))
    wk = nrm(kw[3], (D, HKV * DH), qk / math.sqrt(D))
    wv = nrm(kw[4], (D, HKV * DH), 1.0 / math.sqrt(D))
    wo = nrm(kw[5], (HQ * DH, D), 2.0 / math.sqrt(HQ * DH))
    w1 = nrm(kw[6], (D, F), 1.0 / math.sqrt(D))
    w3 = nrm(kw[7], (D, F), 1.0 / math.sqrt(D))
    w2 = nrm(kw[8], (F, D), 1.0 / math.sqrt(F))
    return dict(x=x, pos=pos, g1=g1, g2=g2, wq=wq, wk=wk, wv=wv, wo=wo, w1=w1, w3=w3, w2=w2)


def rms_norm(v, g):
    vf = v.astype(jnp.float32)
    inv = lax.rsqrt(jnp.mean(vf * vf, axis=-1, keepdims=True) + EPS)
    return (vf * inv * g.astype(jnp.float32)).astype(jnp.bfloat16)


def rope(y, p):
    half = DH // 2
    freq = 1.0 / (THETA ** (jnp.arange(0, DH, 2, dtype=jnp.float32) / DH))
    ang = p.astype(jnp.float32)[..., None] * freq
    c = jnp.cos(ang)[..., None, :]
    s = jnp.sin(ang)[..., None, :]
    y1 = y[..., :half]
    y2 = y[..., half:]
    return jnp.concatenate([y1 * c - y2 * s, y2 * c + y1 * s], axis=-1)


def attention(q, k, v, p):
    qr = q.reshape(T // QB, QB, HKV, GRP, DH)
    pr = p.reshape(T // QB, QB)
    kf = k.astype(jnp.float32)
    vf = v.astype(jnp.float32)
    scale = 1.0 / math.sqrt(DH)

    def blk(qp):
        qq, pp = qp
        s = jnp.einsum('qkgd,skd->kgqs', qq.astype(jnp.float32), kf) * scale
        s = jnp.where(p[None, None, None, :] <= pp[None, None, :, None], s, -1e30)
        e = jnp.exp(s - jnp.max(s, axis=-1, keepdims=True))
        w = (e / jnp.sum(e, axis=-1, keepdims=True)).astype(jnp.bfloat16)
        o = jnp.einsum('kgqs,skd->qkgd', w.astype(jnp.float32), vf)
        return o.astype(jnp.bfloat16)

    return lax.map(blk, (qr, pr)).reshape(T, HQ * DH)


def reference(x, pos, g1, g2, wq, wk, wv, wo, w1, w3, w2):
    a = rms_norm(x, g1)
    q = rope(jnp.dot(a, wq, preferred_element_type=jnp.float32).reshape(T, HQ, DH), pos).astype(jnp.bfloat16)
    k = rope(jnp.dot(a, wk, preferred_element_type=jnp.float32).reshape(T, HKV, DH), pos).astype(jnp.bfloat16)
    v = jnp.dot(a, wv, preferred_element_type=jnp.float32).astype(jnp.bfloat16).reshape(T, HKV, DH)
    o = attention(q, k, v, pos)
    h1 = (x.astype(jnp.float32) + jnp.dot(o, wo, preferred_element_type=jnp.float32)).astype(jnp.bfloat16)
    b = rms_norm(h1, g2)
    hid = (jax.nn.silu(jnp.dot(b, w1, preferred_element_type=jnp.float32)) * jnp.dot(b, w3, preferred_element_type=jnp.float32)).astype(jnp.bfloat16)
    return (h1.astype(jnp.float32) + jnp.dot(hid, w2, preferred_element_type=jnp.float32)).astype(jnp.bfloat16)
```

```python
import math
import jax
import jax.numpy as jnp
from jax import lax
from jax.experimental import pallas as pl
from jax.experimental.pallas import tpu as pltpu
from jax.sharding import PartitionSpec as P

DH = 128
EPS = 1e-5
THETA = 500000.0
D = 3072
HP = 16
HR = 64
QC = 768
KC = 256
FL = 2048
NC = 2
CW = D // NC
MESH = pl.DeviceIdType.MESH
F32 = jnp.float32
BF16 = jnp.bfloat16


def dot(a, b):
    return jnp.dot(a, b, preferred_element_type=F32)


def norm(vf, g):
    inv = lax.rsqrt(jnp.mean(vf * vf, axis=-1, keepdims=True) + EPS)
    return (vf * inv * g).astype(BF16)


def kernel(x_ref, g1_ref, g2_ref, tab_ref, wq_h, wk_h, wv_h, wo_h, w1_h, w3_h, w2_h, out_ref,
           wqkv, wo, w1, w3, w2, ag, tabg, q_s, kv, o_s, hid, pbuf, sbuf, rin, fin, h1_s,
           wsem, ag_s, ag_r, tab_s, tab_r, kv_s, kv_r, rs_s, rin_r, fin_r):
    z = lax.axis_index("tp")
    c = lax.axis_index("cp")
    x = lax.axis_index("dp")

    def at_tp(d):
        return (x, d, c)

    def at_cp(d):
        return (x, z, d)

    side = z // 2
    o = 3 * side
    i = 1 + side
    ip = 2 - side
    op = 3 - 3 * side
    outer = z == o
    inner = z == i
    mate = o + i - z

    wcopies = []
    for n, (src, dst) in enumerate([
        (wq_h, wqkv.at[:, pl.ds(0, QC)]), (wk_h, wqkv.at[:, pl.ds(QC, KC)]), (wv_h, wqkv.at[:, pl.ds(QC + KC, KC)]),
        (wo_h, wo), (w1_h, w1), (w3_h, w3), (w2_h, w2),
    ]):
        cp = pltpu.make_async_copy(src, dst, wsem.at[n])
        cp.start()
        wcopies.append(cp)

    bar = pltpu.get_barrier_semaphore()
    for d in range(1, 4):
        pl.semaphore_signal(bar, inc=1, device_id=at_tp(lax.rem(z + d, 4)), device_id_type=MESH)
        pl.semaphore_signal(bar, inc=1, device_id=at_cp(lax.rem(c + d, 4)), device_id_type=MESH)

    def rows(s, n=HP):
        return pl.ds(pl.multiple_of(s * HP, HP), n)

    outer_sends = []
    inner_sends = []
    all_sends = []

    def ag_copy(ph, slot, dst, k):
        ref = ag.at[ph, rows(slot), :]
        return pltpu.make_async_remote_copy(
            src_ref=ref, dst_ref=ref, send_sem=ag_s.at[ph, k], recv_sem=ag_r.at[ph, slot],
            device_id=at_tp(dst), device_id_type=MESH)

    def ag_send(ph):
        @pl.when(outer)
        def _():
            for k, dst in enumerate((ip, i)):
                ag_copy(ph, z, dst, k).start()

        @pl.when(inner)
        def _():
            for k, dst in enumerate((o, op, ip)):
                ag_copy(ph, z, dst, k).start()

        outer_sends.extend([(lambda k=k, dst=dst: ag_copy(ph, z, dst, k)) for k, dst in enumerate((ip, i))])
        inner_sends.extend([(lambda k=k, dst=dst: ag_copy(ph, z, dst, k)) for k, dst in enumerate((o, op, ip))])
        inner_sends.append(lambda: ag_copy(ph, op, o, 3))

    def ag_relay(ph):
        @pl.when(inner)
        def _():
            ag_copy(ph, op, o, 3).wait_recv()
            ag_copy(ph, op, o, 3).start()

    def ag_wait(ph):
        ag_copy(ph, mate, mate, 0).wait_recv()
        ag_copy(ph, ip, ip, 0).wait_recv()

        @pl.when(outer)
        def _():
            ag_copy(ph, op, op, 0).wait_recv()

    base = rows((1 - side) * 2, 2 * HP)

    def cols(j):
        return pl.ds(j * CW, CW)

    def rs_far(ph, j):
        return pltpu.make_async_remote_copy(
            src_ref=sbuf.at[ph, base, cols(j)], dst_ref=rin.at[ph, :, cols(j)],
            send_sem=rs_s.at[ph, j, 0], recv_sem=rin_r.at[ph, j], device_id=at_tp(mate), device_id_type=MESH)

    def rs_mate(ph, j):
        return pltpu.make_async_remote_copy(
            src_ref=sbuf.at[ph, rows(mate), cols(j)], dst_ref=fin.at[ph, 0, :, cols(j)],
            send_sem=rs_s.at[ph, j, 1], recv_sem=fin_r.at[ph, 0, j], device_id=at_tp(mate), device_id_type=MESH)

    def rs_comb(ph, j, dst, k):
        return pltpu.make_async_remote_copy(
            src_ref=sbuf.at[ph, rows(dst), cols(j)], dst_ref=fin.at[ph, 1, :, cols(j)],
            send_sem=rs_s.at[ph, j, k], recv_sem=fin_r.at[ph, 1, j], device_id=at_tp(dst), device_id_type=MESH)

    def rs_send(ph, lhs, w):
        h = ph % 2
        for j in range(NC):
            part = dot(lhs, w[:, j * CW:(j + 1) * CW])
            pbuf[h, :, j * CW:(j + 1) * CW] = part
            sbuf[ph, :, j * CW:(j + 1) * CW] = part.astype(BF16)

            @pl.when(outer)
            def _():
                rs_far(ph, j).start()

            rs_mate(ph, j).start()
            outer_sends.append(lambda j=j: rs_far(ph, j))
            all_sends.append(lambda j=j: rs_mate(ph, j))
            inner_sends.append(lambda j=j: rs_comb(ph, j, op, 0))
            inner_sends.append(lambda j=j: rs_comb(ph, j, ip, 2))

    def rs_relay(ph):
        h = ph % 2

        @pl.when(inner)
        def _():
            for j in range(NC):
                rs_far(ph, j).wait_recv()
                cs = slice(j * CW, (j + 1) * CW)
                sbuf[ph, base, cs] = (pbuf[h, base, cs] + rin[ph, :, cs].astype(F32)).astype(BF16)
                rs_comb(ph, j, op, 0).start()
                rs_comb(ph, j, ip, 2).start()

    def rs_final(ph):
        h = ph % 2
        for j in range(NC):
            rs_mate(ph, j).wait_recv()
            rs_comb(ph, j, op, 0).wait_recv()
        return pbuf[h, rows(z), :] + fin[ph, 0].astype(F32) + fin[ph, 1].astype(F32)

    def kv_copy(h, slot, dst, k):
        ref = kv.at[h, slot]
        return pltpu.make_async_remote_copy(
            src_ref=ref, dst_ref=ref, send_sem=kv_s.at[h, k], recv_sem=kv_r.at[h, slot],
            device_id=at_cp(dst), device_id_type=MESH)

    def kv_send(h):
        for d in range(1, 4):
            kv_copy(h, c, lax.rem(c + d, 4), d - 1).start()
            all_sends.append(lambda d=d: kv_copy(h, c, lax.rem(c + d, 4), d - 1))

    def kv_wait(h):
        for d in range(1, 4):
            s = lax.rem(c + d, 4)
            kv_copy(h, s, s, 0).wait_recv()

    def tab_copy(slot, dst, k):
        return pltpu.make_async_remote_copy(
            src_ref=tab_ref, dst_ref=tabg.at[slot], send_sem=tab_s.at[k], recv_sem=tab_r.at[slot],
            device_id=at_tp(dst), device_id_type=MESH)

    def qkv(h):
        a = ag[h]
        t = tabg[:, h * HP:(h + 1) * HP, :].reshape(HR, DH)
        r = pltpu.roll(t, DH // 2, 1)
        low = lax.broadcasted_iota(jnp.int32, (HR, DH), 1) < DH // 2
        cos = jnp.where(low, t, r)
        sin = jnp.where(low, -r, t)

        def rope(y):
            return (y * cos + pltpu.roll(y, DH // 2, 1) * sin).astype(BF16)

        y = dot(a, wqkv[:, QC:])
        for n in range(2):
            kv[h, c, :, n * DH:(n + 1) * DH] = rope(y[:, n * DH:(n + 1) * DH])
        kv[h, c, :, KC:] = y[:, KC:].astype(BF16)
        kv_send(h)
        y = dot(a, wqkv[:, :QC])
        for n in range(6):
            q_s[h, :, n * DH:(n + 1) * DH] = rope(y[:, n * DH:(n + 1) * DH])

    scale = 1.0 / math.sqrt(DH)

    def dotT(a, b):
        return lax.dot_general(a, b, (((1,), (1,)), ((), ())), preferred_element_type=F32)

    def attn(h):
        nq = 3 * HR
        f = lax.broadcasted_iota(jnp.int32, (nq, 4 * HR), 0) & (HR - 1)
        kk = lax.broadcasted_iota(jnp.int32, (nq, 4 * HR), 1)
        if h == 0:
            seen = kk <= c * HR + f
        else:
            seq_q = (31 - 4 * c - (f >> 4)) * HP + (f & (HP - 1))
            seq_k = (31 - (kk >> 4)) * HP + (kk & (HP - 1))
            seen = seq_k <= seq_q
        for g in range(2):
            qg = jnp.concatenate([q_s[h, :, (3 * g + t) * DH:(3 * g + t + 1) * DH] for t in range(3)], axis=0)
            ks = [kv[e, :, :, g * DH:(g + 1) * DH].reshape(4 * HR, DH) for e in range(h + 1)]
            vs = [kv[e, :, :, KC + g * DH:KC + (g + 1) * DH].reshape(4 * HR, DH) for e in range(h + 1)]
            ss = [dotT(qg, k) * scale for k in ks]
            ss[h] = jnp.where(seen, ss[h], -1e30)
            m = jnp.max(ss[0], axis=-1, keepdims=True)
            for s in ss[1:]:
                m = jnp.maximum(m, jnp.max(s, axis=-1, keepdims=True))
            es = [jnp.exp(s - m) for s in ss]
            tot = jnp.sum(es[0], axis=-1, keepdims=True)
            for e in es[1:]:
                tot = tot + jnp.sum(e, axis=-1, keepdims=True)
            inv = 1.0 / tot
            acc = None
            for e, v in zip(es, vs):
                t = dot((e * inv).astype(BF16), v)
                acc = t if acc is None else acc + t
            for t in range(3):
                o_s[h, :, (3 * g + t) * DH:(3 * g + t + 1) * DH] = acc[t * HR:(t + 1) * HR].astype(BF16)

    def mlp_up(h):
        b = ag[2 + h]
        for n in range(4):
            cs = slice(n * 512, (n + 1) * 512)
            gate = dot(b, w1[:, cs])
            up = dot(b, w3[:, cs])
            hid[:, cs] = (jax.nn.silu(gate) * up).astype(BF16)

    def h1_final(h):
        y = rs_final(h)
        h1 = (x_ref[h * HP:(h + 1) * HP, :].astype(F32) + y).astype(BF16)
        h1_s[h] = h1
        ag[2 + h, rows(z), :] = norm(h1.astype(F32), g2_ref[...].astype(F32))
        ag_send(2 + h)

    def out_final(h):
        y = rs_final(2 + h)
        out_ref[h * HP:(h + 1) * HP, :] = (h1_s[h].astype(F32) + y).astype(BF16)

    a = norm(x_ref[...].astype(F32), g1_ref[...].astype(F32))
    for h in range(2):
        ag[h, rows(z), :] = a[h * HP:(h + 1) * HP]
    tabg[z] = tab_ref[...]
    pl.semaphore_wait(bar, 6)
    ag_send(0)
    for d in range(1, 4):
        tab_copy(z, lax.rem(z + d, 4), d - 1).start()
        all_sends.append(lambda d=d: tab_copy(z, lax.rem(z + d, 4), d - 1))
    ag_send(1)

    ag_relay(0)
    ag_wait(0)
    for d in range(1, 4):
        s = lax.rem(z + d, 4)
        tab_copy(s, s, 0).wait_recv()
    for n in range(3):
        wcopies[n].wait()
    qkv(0)
    ag_relay(1)
    ag_wait(1)
    qkv(1)
    kv_wait(0)
    attn(0)
    wcopies[3].wait()
    rs_send(0, o_s[0], wo)
    kv_wait(1)
    attn(1)
    rs_relay(0)
    rs_send(1, o_s[1], wo)
    h1_final(0)
    rs_relay(1)
    ag_relay(2)
    h1_final(1)
    ag_wait(2)
    for n in range(4, 7):
        wcopies[n].wait()
    mlp_up(0)
    ag_relay(3)
    rs_send(2, hid[...], w2)
    ag_wait(3)
    mlp_up(1)
    rs_relay(2)
    rs_send(3, hid[...], w2)
    out_final(0)
    rs_relay(3)
    out_final(1)

    for s in all_sends:
        s().wait_send()

    @pl.when(outer)
    def _():
        for s in outer_sends:
            s().wait_send()

    @pl.when(inner)
    def _():
        for s in inner_sends:
            s().wait_send()


def layer(x, g1, g2, tab, wq, wk, wv, wo, w1, w3, w2):
    vm = pl.BlockSpec(memory_space=pltpu.VMEM)
    hb = pl.BlockSpec(memory_space=pl.ANY)
    dma = pltpu.SemaphoreType.DMA
    return pl.pallas_call(
        kernel,
        out_shape=jax.ShapeDtypeStruct((2 * HP, D), BF16),
        in_specs=[vm] * 4 + [hb] * 7,
        out_specs=vm,
        scratch_shapes=[
            pltpu.VMEM((D, QC + 2 * KC), BF16),
            pltpu.VMEM((QC, D), BF16),
            pltpu.VMEM((D, FL), BF16),
            pltpu.VMEM((D, FL), BF16),
            pltpu.VMEM((FL, D), BF16),
            pltpu.VMEM((4, HR, D), BF16),
            pltpu.VMEM((4, 2 * HP, DH), F32),
            pltpu.VMEM((2, HR, QC), BF16),
            pltpu.VMEM((2, 4, HR, 2 * KC), BF16),
            pltpu.VMEM((2, HR, QC), BF16),
            pltpu.VMEM((HR, FL), BF16),
            pltpu.VMEM((2, HR, D), F32),
            pltpu.VMEM((4, HR, D), BF16),
            pltpu.VMEM((4, 2 * HP, D), BF16),
            pltpu.VMEM((4, 2, HP, D), BF16),
            pltpu.VMEM((2, HP, D), BF16),
            dma((7,)),
            dma((4, 4)),
            dma((4, 4)),
            dma((3,)),
            dma((4,)),
            dma((2, 3)),
            dma((2, 4)),
            dma((4, NC, 3)),
            dma((4, NC)),
            dma((4, 2, NC)),
        ],
        compiler_params=pltpu.CompilerParams(
            collective_id=0, has_side_effects=True, vmem_limit_bytes=67043328),
        name="layer",
    )(x, g1, g2, tab, wq, wk, wv, wo, w1, w3, w2)


def solution(mesh):
    tok = P(('dp', 'cp', 'tp'), None)
    col = P(None, 'tp')
    row = P('tp', None)

    def local(x, pos, g1, g2, wq, wk, wv, wo, w1, w3, w2):
        freq = 1.0 / (THETA ** (jnp.arange(0, DH, 2, dtype=F32) / DH))
        ang = pos.astype(F32)[:, None] * freq
        tab = jnp.concatenate([jnp.cos(ang), jnp.sin(ang)], axis=-1)
        return layer(x, g1.reshape(1, D), g2.reshape(1, D), tab, wq, wk, wv, wo, w1, w3, w2)

    return jax.shard_map(local, mesh=mesh, in_specs=(tok, P(('dp', 'cp', 'tp')), P(None), P(None), col, col, col, row, col, col, row), out_specs=tok, check_vma=False)
```

```python
import math
import jax
import numpy as np
import jax.numpy as jnp
from jax import lax
from jax.experimental import pallas as pl
from jax.experimental.pallas import tpu as pltpu
from jax.sharding import PartitionSpec as P

DH = 128
EPS = 1e-5
THETA = 500000.0
D = 3072
HP = 16
HR = 64
QC = 768
KC = 256
FL = 2048
NC = 3
CW = D // NC
MESH = pl.DeviceIdType.MESH
F32 = jnp.float32
BF16 = jnp.bfloat16


def dot(a, b):
    return jnp.dot(a, b, preferred_element_type=F32)


def norm(vf, g):
    inv = lax.rsqrt(jnp.mean(vf * vf, axis=-1, keepdims=True) + EPS)
    return (vf * inv * g).astype(BF16)


def gain(ref):
    g = ref[...].astype(F32)
    return jnp.concatenate([g[n:n + 1] for n in range(D // DH)], axis=1)


def kernel(x_ref, pos_ref, freq_ref, g1_ref, g2_ref, wq_h, wk_h, wv_h, wo_h, w1_h, w3_h, w2_h, out_ref,
           wqkv, wo, w1, w3, w2, ag, tab_own, tabg, q_s, kv, o_s, hid, pbuf, sbuf, rin, fin, h1_s,
           wsem, ag_s, ag_r, tab_s, tab_r, kv_s, kv_r, rs_s, rin_r, fin_r):
    z = lax.axis_index("tp")
    c = lax.axis_index("cp")
    x = lax.axis_index("dp")

    def at_tp(d):
        return (x, d, c)

    def at_cp(d):
        return (x, z, d)

    side = z // 2
    o = 3 * side
    i = 1 + side
    ip = 2 - side
    op = 3 - 3 * side
    outer = z == o
    inner = z == i
    mate = o + i - z

    wcopies = []
    for n, (src, dst) in enumerate([
        (wq_h, wqkv.at[:, pl.ds(0, QC)]), (wk_h, wqkv.at[:, pl.ds(QC, KC)]), (wv_h, wqkv.at[:, pl.ds(QC + KC, KC)]),
        (wo_h, wo), (w1_h, w1), (w3_h, w3), (w2_h, w2),
    ]):
        cp = pltpu.make_async_copy(src, dst, wsem.at[n])
        cp.start()
        wcopies.append(cp)

    bar = pltpu.get_barrier_semaphore()
    for d in range(1, 4):
        pl.semaphore_signal(bar, inc=1, device_id=at_tp(lax.rem(z + d, 4)), device_id_type=MESH)
        pl.semaphore_signal(bar, inc=1, device_id=at_cp(lax.rem(c + d, 4)), device_id_type=MESH)

    def rows(s, n=HP):
        return pl.ds(pl.multiple_of(s * HP, HP), n)

    outer_sends = []
    inner_sends = []
    all_sends = []

    def ag_copy(ph, slot, dst, k):
        ref = ag.at[ph, rows(slot), :]
        return pltpu.make_async_remote_copy(
            src_ref=ref, dst_ref=ref, send_sem=ag_s.at[ph, k], recv_sem=ag_r.at[ph, slot],
            device_id=at_tp(dst), device_id_type=MESH)

    def ag_send(ph):
        @pl.when(outer)
        def _():
            for k, dst in enumerate((ip, i)):
                ag_copy(ph, z, dst, k).start()

        @pl.when(inner)
        def _():
            for k, dst in enumerate((o, op, ip)):
                ag_copy(ph, z, dst, k).start()

        outer_sends.extend([(lambda k=k, dst=dst: ag_copy(ph, z, dst, k)) for k, dst in enumerate((ip, i))])
        inner_sends.extend([(lambda k=k, dst=dst: ag_copy(ph, z, dst, k)) for k, dst in enumerate((o, op, ip))])
        inner_sends.append(lambda: ag_copy(ph, op, o, 3))

    def ag_relay(ph):
        @pl.when(inner)
        def _():
            ag_copy(ph, op, o, 3).wait_recv()
            ag_copy(ph, op, o, 3).start()

    def ag_wait(ph):
        ag_copy(ph, mate, mate, 0).wait_recv()
        ag_copy(ph, ip, ip, 0).wait_recv()

        @pl.when(outer)
        def _():
            ag_copy(ph, op, op, 0).wait_recv()

    base = rows((1 - side) * 2, 2 * HP)

    def cols(j):
        return pl.ds(j * CW, CW)

    def rs_far(ph, j):
        return pltpu.make_async_remote_copy(
            src_ref=sbuf.at[ph, base, cols(j)], dst_ref=rin.at[ph, :, cols(j)],
            send_sem=rs_s.at[ph, j, 0], recv_sem=rin_r.at[ph, j], device_id=at_tp(mate), device_id_type=MESH)

    def rs_mate(ph):
        return pltpu.make_async_remote_copy(
            src_ref=sbuf.at[ph, rows(mate), :], dst_ref=fin.at[ph, 0],
            send_sem=rs_s.at[ph, NC, 0], recv_sem=fin_r.at[ph, 0, 0], device_id=at_tp(mate), device_id_type=MESH)

    def rs_comb(ph, j, dst, k):
        return pltpu.make_async_remote_copy(
            src_ref=sbuf.at[ph, rows(dst), cols(j)], dst_ref=fin.at[ph, 1, :, cols(j)],
            send_sem=rs_s.at[ph, j, 1 + k], recv_sem=fin_r.at[ph, 1, j], device_id=at_tp(dst), device_id_type=MESH)

    def rs_send(ph, lhs, w, js=range(NC)):
        h = ph % 2
        for j in js:
            part = dot(lhs, w[:, j * CW:(j + 1) * CW])
            pbuf[h, :, j * CW:(j + 1) * CW] = part
            sbuf[ph, :, j * CW:(j + 1) * CW] = part.astype(BF16)

            @pl.when(outer)
            def _():
                rs_far(ph, j).start()

            outer_sends.append(lambda j=j: rs_far(ph, j))
            inner_sends.append(lambda j=j: rs_comb(ph, j, op, 0))
            inner_sends.append(lambda j=j: rs_comb(ph, j, ip, 1))
        if js[-1] == NC - 1:
            rs_mate(ph).start()
            all_sends.append(lambda: rs_mate(ph))

    def rs_relay(ph):
        h = ph % 2

        @pl.when(inner)
        def _():
            for j in range(NC):
                rs_far(ph, j).wait_recv()
                cs = slice(j * CW, (j + 1) * CW)
                sbuf[ph, base, cs] = (pbuf[h, base, cs] + rin[ph, :, cs].astype(F32)).astype(BF16)
                rs_comb(ph, j, op, 0).start()
                rs_comb(ph, j, ip, 1).start()

    def rs_final(ph):
        h = ph % 2
        rs_mate(ph).wait_recv()
        for j in range(NC):
            rs_comb(ph, j, op, 0).wait_recv()
        return pbuf[h, rows(z), :] + fin[ph, 0].astype(F32) + fin[ph, 1].astype(F32)

    def kv_copy(h, slot, dst, k):
        ref = kv.at[h, slot]
        return pltpu.make_async_remote_copy(
            src_ref=ref, dst_ref=ref, send_sem=kv_s.at[h, k], recv_sem=kv_r.at[h, slot],
            device_id=at_cp(dst), device_id_type=MESH)

    def kv_send(h):
        for d in range(1, 4):
            kv_copy(h, c, lax.rem(c + d, 4), d - 1).start()
            all_sends.append(lambda d=d: kv_copy(h, c, lax.rem(c + d, 4), d - 1))

    def kv_wait(h):
        for d in range(1, 4):
            s = lax.rem(c + d, 4)
            kv_copy(h, s, s, 0).wait_recv()

    def tab_copy(slot, dst, k):
        return pltpu.make_async_remote_copy(
            src_ref=tab_own, dst_ref=tabg.at[slot], send_sem=tab_s.at[k], recv_sem=tab_r.at[slot],
            device_id=at_tp(dst), device_id_type=MESH)

    def qkv(h):
        a = ag[h]
        t = tabg[:, h * HP:(h + 1) * HP, :].reshape(HR, DH)
        r = pltpu.roll(t, DH // 2, 1)
        low = lax.broadcasted_iota(jnp.int32, (HR, DH), 1) < DH // 2
        cos = jnp.where(low, t, r)
        sin = jnp.where(low, -r, t)

        def rope(y):
            return (y * cos + pltpu.roll(y, DH // 2, 1) * sin).astype(BF16)

        y = dot(a, wqkv[:, QC:])
        for n in range(2):
            kv[h, c, :, n * DH:(n + 1) * DH] = rope(y[:, n * DH:(n + 1) * DH])
        kv[h, c, :, KC:] = y[:, KC:].astype(BF16)
        kv_send(h)
        y = dot(a, wqkv[:, :QC])
        for n in range(6):
            q_s[h, :, n * DH:(n + 1) * DH] = rope(y[:, n * DH:(n + 1) * DH])

    scale = 1.0 / math.sqrt(DH)

    def dotT(a, b):
        return lax.dot_general(a, b, (((1,), (1,)), ((), ())), preferred_element_type=F32)

    def attn(h):
        nq = 3 * HR
        f = lax.broadcasted_iota(jnp.int32, (nq, 4 * HR), 0) & (HR - 1)
        kk = lax.broadcasted_iota(jnp.int32, (nq, 4 * HR), 1)
        if h == 0:
            seen = kk <= c * HR + f
        else:
            seq_q = (31 - 4 * c - (f >> 4)) * HP + (f & (HP - 1))
            seq_k = (31 - (kk >> 4)) * HP + (kk & (HP - 1))
            seen = seq_k <= seq_q
        for g in range(2):
            qg = jnp.concatenate([q_s[h, :, (3 * g + t) * DH:(3 * g + t + 1) * DH] for t in range(3)], axis=0)
            ks = [kv[e, :, :, g * DH:(g + 1) * DH].reshape(4 * HR, DH) for e in range(h + 1)]
            vs = [kv[e, :, :, KC + g * DH:KC + (g + 1) * DH].reshape(4 * HR, DH) for e in range(h + 1)]
            ss = [dotT(qg, k) * scale for k in ks]
            ss[h] = jnp.where(seen, ss[h], -1e30)
            m = jnp.max(ss[0], axis=-1, keepdims=True)
            for s in ss[1:]:
                m = jnp.maximum(m, jnp.max(s, axis=-1, keepdims=True))
            es = [jnp.exp(s - m) for s in ss]
            tot = jnp.sum(es[0], axis=-1, keepdims=True)
            for e in es[1:]:
                tot = tot + jnp.sum(e, axis=-1, keepdims=True)
            inv = 1.0 / tot
            acc = None
            for e, v in zip(es, vs):
                t = dot((e * inv).astype(BF16), v)
                acc = t if acc is None else acc + t
            for t in range(3):
                o_s[h, :, (3 * g + t) * DH:(3 * g + t + 1) * DH] = acc[t * HR:(t + 1) * HR].astype(BF16)

    def mlp_up(h):
        b = ag[2 + h]
        for n in range(4):
            cs = slice(n * 512, (n + 1) * 512)
            gate = dot(b, w1[:, cs])
            up = dot(b, w3[:, cs])
            hid[:, cs] = (jax.nn.silu(gate) * up).astype(BF16)

    def h1_final(h):
        y = rs_final(h)
        h1 = (x_ref[h * HP:(h + 1) * HP, :].astype(F32) + y).astype(BF16)
        h1_s[h] = h1
        ag[2 + h, rows(z), :] = norm(h1.astype(F32), gain(g2_ref))
        ag_send(2 + h)

    def out_final(h):
        y = rs_final(2 + h)
        out_ref[h * HP:(h + 1) * HP, :] = (h1_s[h].astype(F32) + y).astype(BF16)

    def table():
        p = jnp.broadcast_to(pos_ref[...].astype(F32).reshape(1, 2 * HP), (2 * HP, 2 * HP))
        r = lax.broadcasted_iota(jnp.int32, (2 * HP, 2 * HP), 0)
        k = lax.broadcasted_iota(jnp.int32, (2 * HP, 2 * HP), 1)
        p = jnp.sum(jnp.where(r == k, p, 0.0), axis=1, keepdims=True)
        ang = p * freq_ref[...]
        low = lax.broadcasted_iota(jnp.int32, (2 * HP, DH), 1) < DH // 2
        return jnp.where(low, jnp.cos(ang), jnp.sin(ang))

    sc = jax.named_scope
    with sc("start"):
        a = norm(x_ref[...].astype(F32), gain(g1_ref))
        for h in range(2):
            ag[h, rows(z), :] = a[h * HP:(h + 1) * HP]
        t = table()
        tab_own[...] = t
        tabg[z] = t
    with sc("bar"):
        pl.semaphore_wait(bar, 6)
    with sc("send0"):
        for d in range(1, 4):
            tab_copy(z, lax.rem(z + d, 4), d - 1).start()
            all_sends.append(lambda d=d: tab_copy(z, lax.rem(z + d, 4), d - 1))
        ag_send(0)
        ag_send(1)
    with sc("agrelay0"):
        ag_relay(0)
    with sc("agwait0"):
        ag_wait(0)
    with sc("tabwait"):
        for d in range(1, 4):
            s = lax.rem(z + d, 4)
            tab_copy(s, s, 0).wait_recv()
    with sc("wqkv"):
        for n in range(3):
            wcopies[n].wait()
    with sc("qkv0"):
        qkv(0)
    with sc("agrelay1"):
        ag_relay(1)
    with sc("kvwait0"):
        kv_wait(0)
    with sc("attn0"):
        attn(0)
    with sc("wowait"):
        wcopies[3].wait()
    with sc("rssend0"):
        rs_send(0, o_s[0], wo)
    with sc("agwait1"):
        ag_wait(1)
    with sc("qkv1"):
        qkv(1)
    with sc("rsrelay0"):
        rs_relay(0)
    with sc("kvwait1"):
        kv_wait(1)
    with sc("attn1"):
        attn(1)
    with sc("rssend1"):
        rs_send(1, o_s[1], wo)
    with sc("h1final0"):
        h1_final(0)
    with sc("agrelay2"):
        ag_relay(2)
    with sc("rsrelay1"):
        rs_relay(1)
    with sc("h1final1"):
        h1_final(1)
    with sc("agwait2"):
        ag_wait(2)
    with sc("wmlp"):
        for n in range(4, 7):
            wcopies[n].wait()
    with sc("mlp0"):
        mlp_up(0)
    with sc("rssend2"):
        rs_send(2, hid[...], w2, range(0, 2))
    with sc("agrelay3"):
        ag_relay(3)
    with sc("rssend2b"):
        rs_send(2, hid[...], w2, range(2, 3))
    with sc("agwait3"):
        ag_wait(3)
    with sc("mlp1"):
        mlp_up(1)
    with sc("rsrelay2"):
        rs_relay(2)
    with sc("rssend3"):
        rs_send(3, hid[...], w2)
    with sc("outfinal0"):
        out_final(0)
    with sc("rsrelay3"):
        rs_relay(3)
    with sc("outfinal1"):
        out_final(1)

    for s in all_sends:
        s().wait_send()

    @pl.when(outer)
    def _():
        for s in outer_sends:
            s().wait_send()

    @pl.when(inner)
    def _():
        for s in inner_sends:
            s().wait_send()


def layer(x, pos, freq, g1, g2, wq, wk, wv, wo, w1, w3, w2):
    vm = pl.BlockSpec(memory_space=pltpu.VMEM)
    hb = pl.BlockSpec(memory_space=pl.ANY)
    dma = pltpu.SemaphoreType.DMA
    return pl.pallas_call(
        kernel,
        out_shape=jax.ShapeDtypeStruct((2 * HP, D), BF16),
        in_specs=[vm] * 5 + [hb] * 7,
        out_specs=vm,
        scratch_shapes=[
            pltpu.VMEM((D, QC + 2 * KC), BF16),
            pltpu.VMEM((QC, D), BF16),
            pltpu.VMEM((D, FL), BF16),
            pltpu.VMEM((D, FL), BF16),
            pltpu.VMEM((FL, D), BF16),
            pltpu.VMEM((4, HR, D), BF16),
            pltpu.VMEM((2 * HP, DH), F32),
            pltpu.VMEM((4, 2 * HP, DH), F32),
            pltpu.VMEM((2, HR, QC), BF16),
            pltpu.VMEM((2, 4, HR, 2 * KC), BF16),
            pltpu.VMEM((2, HR, QC), BF16),
            pltpu.VMEM((HR, FL), BF16),
            pltpu.VMEM((2, HR, D), F32),
            pltpu.VMEM((4, HR, D), BF16),
            pltpu.VMEM((4, 2 * HP, D), BF16),
            pltpu.VMEM((4, 2, HP, D), BF16),
            pltpu.VMEM((2, HP, D), BF16),
            dma((7,)),
            dma((4, 4)),
            dma((4, 4)),
            dma((3,)),
            dma((4,)),
            dma((2, 3)),
            dma((2, 4)),
            dma((4, NC + 1, 3)),
            dma((4, NC)),
            dma((4, 2, NC)),
        ],
        compiler_params=pltpu.CompilerParams(
            collective_id=0, has_side_effects=True, vmem_limit_bytes=58 * 2**20),
        name="layer",
    )(x, pos, freq, g1, g2, wq, wk, wv, wo, w1, w3, w2)


def solution(mesh):
    tok = P(('dp', 'cp', 'tp'), None)
    col = P(None, 'tp')
    row = P('tp', None)

    def local(x, pos, g1, g2, wq, wk, wv, wo, w1, w3, w2):
        f = 1.0 / THETA ** (np.arange(0, DH, 2) / DH)
        freq = jnp.asarray(np.concatenate([f, f])[None].astype(np.float32))
        return layer(x, pos, freq, g1.reshape(D // DH, DH), g2.reshape(D // DH, DH), wq, wk, wv, wo, w1, w3, w2)

    return jax.shard_map(local, mesh=mesh, in_specs=(tok, P(('dp', 'cp', 'tp')), P(None), P(None), col, col, col, row, col, col, row), out_specs=tok, check_vma=False)
```

```python
import math
import jax
import numpy as np
import jax.numpy as jnp
from jax import lax
from jax.experimental import pallas as pl
from jax.experimental.pallas import tpu as pltpu
from jax.sharding import PartitionSpec as P

DH = 128
EPS = 1e-5
THETA = 500000.0
D = 3072
HP = 16
HR = 64
QC = 768
KC = 256
FL = 2048
NC = 3
CW = D // NC
MESH = pl.DeviceIdType.MESH
F32 = jnp.float32
BF16 = jnp.bfloat16


def dot(a, b):
    return jnp.dot(a, b, preferred_element_type=F32)


def norm(vf, g):
    inv = lax.rsqrt(jnp.mean(vf * vf, axis=-1, keepdims=True) + EPS)
    return (vf * inv * g).astype(BF16)


def gain(ref):
    g = ref[...].astype(F32)
    return jnp.concatenate([g[n:n + 1] for n in range(D // DH)], axis=1)


def kernel(x_h, pos_h, freq_h, g1_h, g2_h, wq_h, wk_h, wv_h, wo_h, w1_h, w3_h, w2_h, out_ref,
           x_ref, pos_ref, freq_ref, g1_ref, g2_ref, wqkv, wo, w1, w3, w2, ag, tab_own, tabg, q_s, kv, o_s, hid, pbuf, sbuf, rin, fin, h1_s,
           xsem, wsem, ag_s, ag_r, tab_s, tab_r, kv_s, kv_r, rs_s, rin_r, fin_r):
    z = lax.axis_index("tp")
    c = lax.axis_index("cp")
    x = lax.axis_index("dp")

    def at_tp(d):
        return (x, d, c)

    def at_cp(d):
        return (x, z, d)

    side = z // 2
    o = 3 * side
    i = 1 + side
    ip = 2 - side
    op = 3 - 3 * side
    outer = z == o
    inner = z == i
    mate = o + i - z

    icopies = [pltpu.make_async_copy(src, dst, xsem.at[n]) for n, (src, dst) in enumerate([
        (x_h, x_ref), (g1_h, g1_ref), (pos_h, pos_ref), (freq_h, freq_ref), (g2_h, g2_ref)])]
    icopies[0].start()
    icopies[1].start()
    bar = pltpu.get_barrier_semaphore()
    for d in range(1, 4):
        pl.semaphore_signal(bar, inc=1, device_id=at_tp(lax.rem(z + d, 4)), device_id_type=MESH)
        pl.semaphore_signal(bar, inc=1, device_id=at_cp(lax.rem(c + d, 4)), device_id_type=MESH)
    for cp in icopies[2:]:
        cp.start()

    wcopies = []
    for n, (src, dst) in enumerate([
        (wq_h, wqkv.at[:, pl.ds(0, QC)]), (wk_h, wqkv.at[:, pl.ds(QC, KC)]), (wv_h, wqkv.at[:, pl.ds(QC + KC, KC)]),
        (wo_h, wo), (w1_h, w1), (w3_h, w3), (w2_h, w2),
    ]):
        cp = pltpu.make_async_copy(src, dst, wsem.at[n])
        cp.start()
        wcopies.append(cp)

    def rows(s, n=HP):
        return pl.ds(pl.multiple_of(s * HP, HP), n)

    outer_sends = []
    inner_sends = []
    all_sends = []

    def ag_copy(ph, slot, dst, k):
        ref = ag.at[ph, rows(slot), :]
        return pltpu.make_async_remote_copy(
            src_ref=ref, dst_ref=ref, send_sem=ag_s.at[ph, k], recv_sem=ag_r.at[ph, slot],
            device_id=at_tp(dst), device_id_type=MESH)

    def ag_send(ph):
        @pl.when(outer)
        def _():
            for k, dst in enumerate((ip, i)):
                ag_copy(ph, z, dst, k).start()

        @pl.when(inner)
        def _():
            for k, dst in enumerate((o, op, ip)):
                ag_copy(ph, z, dst, k).start()

        outer_sends.extend([(lambda k=k, dst=dst: ag_copy(ph, z, dst, k)) for k, dst in enumerate((ip, i))])
        inner_sends.extend([(lambda k=k, dst=dst: ag_copy(ph, z, dst, k)) for k, dst in enumerate((o, op, ip))])
        inner_sends.append(lambda: ag_copy(ph, op, o, 3))

    def ag_relay(ph):
        @pl.when(inner)
        def _():
            ag_copy(ph, op, o, 3).wait_recv()
            ag_copy(ph, op, o, 3).start()

    def ag_wait(ph):
        ag_copy(ph, mate, mate, 0).wait_recv()
        ag_copy(ph, ip, ip, 0).wait_recv()

        @pl.when(outer)
        def _():
            ag_copy(ph, op, op, 0).wait_recv()

    base = rows((1 - side) * 2, 2 * HP)

    def cols(j):
        return pl.ds(j * CW, CW)

    def rs_far(ph, j):
        return pltpu.make_async_remote_copy(
            src_ref=sbuf.at[ph, base, cols(j)], dst_ref=rin.at[ph, :, cols(j)],
            send_sem=rs_s.at[ph, j, 0], recv_sem=rin_r.at[ph, j], device_id=at_tp(mate), device_id_type=MESH)

    def rs_mate(ph):
        return pltpu.make_async_remote_copy(
            src_ref=sbuf.at[ph, rows(mate), :], dst_ref=fin.at[ph, 0],
            send_sem=rs_s.at[ph, NC, 0], recv_sem=fin_r.at[ph, 0, 0], device_id=at_tp(mate), device_id_type=MESH)

    def rs_comb(ph, j, dst, k):
        return pltpu.make_async_remote_copy(
            src_ref=sbuf.at[ph, rows(dst), cols(j)], dst_ref=fin.at[ph, 1, :, cols(j)],
            send_sem=rs_s.at[ph, j, 1 + k], recv_sem=fin_r.at[ph, 1, j], device_id=at_tp(dst), device_id_type=MESH)

    def rs_send(ph, lhs, w, js=range(NC)):
        h = ph % 2
        for j in js:
            part = dot(lhs, w[:, j * CW:(j + 1) * CW])
            pbuf[h, :, j * CW:(j + 1) * CW] = part
            sbuf[ph, :, j * CW:(j + 1) * CW] = part.astype(BF16)

            @pl.when(outer)
            def _():
                rs_far(ph, j).start()

            outer_sends.append(lambda j=j: rs_far(ph, j))
            inner_sends.append(lambda j=j: rs_comb(ph, j, op, 0))
            inner_sends.append(lambda j=j: rs_comb(ph, j, ip, 1))
        all_sends.extend([lambda: rs_mate(ph)] if js[-1] == NC - 1 else [])

    def rs_relay(ph):
        h = ph % 2

        @pl.when(inner)
        def _():
            for j in range(NC):
                rs_far(ph, j).wait_recv()
                cs = slice(j * CW, (j + 1) * CW)
                sbuf[ph, base, cs] = (pbuf[h, base, cs] + rin[ph, :, cs].astype(F32)).astype(BF16)
                rs_comb(ph, j, op, 0).start()
                rs_comb(ph, j, ip, 1).start()

    def rs_final(ph):
        h = ph % 2
        rs_mate(ph).wait_recv()
        for j in range(NC):
            rs_comb(ph, j, op, 0).wait_recv()
        return pbuf[h, rows(z), :] + fin[ph, 0].astype(F32) + fin[ph, 1].astype(F32)

    def kv_copy(h, slot, dst, k):
        ref = kv.at[h, slot]
        return pltpu.make_async_remote_copy(
            src_ref=ref, dst_ref=ref, send_sem=kv_s.at[h, k], recv_sem=kv_r.at[h, slot],
            device_id=at_cp(dst), device_id_type=MESH)

    def kv_send(h):
        for d in range(1, 4):
            kv_copy(h, c, lax.rem(c + d, 4), d - 1).start()
            all_sends.append(lambda d=d: kv_copy(h, c, lax.rem(c + d, 4), d - 1))

    def kv_wait(h):
        for d in range(1, 4):
            s = lax.rem(c + d, 4)
            kv_copy(h, s, s, 0).wait_recv()

    def tab_copy(slot, dst, k):
        return pltpu.make_async_remote_copy(
            src_ref=tab_own, dst_ref=tabg.at[slot], send_sem=tab_s.at[k], recv_sem=tab_r.at[slot],
            device_id=at_tp(dst), device_id_type=MESH)

    def qkv(h):
        a = ag[h]
        t = tabg[:, h * HP:(h + 1) * HP, :].reshape(HR, DH)
        r = pltpu.roll(t, DH // 2, 1)
        low = lax.broadcasted_iota(jnp.int32, (HR, DH), 1) < DH // 2
        cos = jnp.where(low, t, r)
        sin = jnp.where(low, -r, t)

        def rope(y):
            return (y * cos + pltpu.roll(y, DH // 2, 1) * sin).astype(BF16)

        y = dot(a, wqkv[:, QC:])
        for n in range(2):
            kv[h, c, :, n * DH:(n + 1) * DH] = rope(y[:, n * DH:(n + 1) * DH])
        kv[h, c, :, KC:] = y[:, KC:].astype(BF16)
        kv_send(h)
        y = dot(a, wqkv[:, :QC])
        for n in range(6):
            q_s[h, :, n * DH:(n + 1) * DH] = rope(y[:, n * DH:(n + 1) * DH])

    scale = 1.0 / math.sqrt(DH)

    def dotT(a, b):
        return lax.dot_general(a, b, (((1,), (1,)), ((), ())), preferred_element_type=F32)

    def attn(h):
        nq = 3 * HR
        f = lax.broadcasted_iota(jnp.int32, (nq, 4 * HR), 0) & (HR - 1)
        kk = lax.broadcasted_iota(jnp.int32, (nq, 4 * HR), 1)
        if h == 0:
            seen = kk <= c * HR + f
        else:
            seq_q = (31 - 4 * c - (f >> 4)) * HP + (f & (HP - 1))
            seq_k = (31 - (kk >> 4)) * HP + (kk & (HP - 1))
            seen = seq_k <= seq_q
        for g in range(2):
            qg = jnp.concatenate([q_s[h, :, (3 * g + t) * DH:(3 * g + t + 1) * DH] for t in range(3)], axis=0)
            ks = [kv[e, :, :, g * DH:(g + 1) * DH].reshape(4 * HR, DH) for e in range(h + 1)]
            vs = [kv[e, :, :, KC + g * DH:KC + (g + 1) * DH].reshape(4 * HR, DH) for e in range(h + 1)]
            ss = [dotT(qg, k) * scale for k in ks]
            ss[h] = jnp.where(seen, ss[h], -1e30)
            m = jnp.max(ss[0], axis=-1, keepdims=True)
            for s in ss[1:]:
                m = jnp.maximum(m, jnp.max(s, axis=-1, keepdims=True))
            es = [jnp.exp(s - m) for s in ss]
            tot = jnp.sum(es[0], axis=-1, keepdims=True)
            for e in es[1:]:
                tot = tot + jnp.sum(e, axis=-1, keepdims=True)
            inv = 1.0 / tot
            acc = None
            for e, v in zip(es, vs):
                t = dot((e * inv).astype(BF16), v)
                acc = t if acc is None else acc + t
            for t in range(3):
                o_s[h, :, (3 * g + t) * DH:(3 * g + t + 1) * DH] = acc[t * HR:(t + 1) * HR].astype(BF16)

    def mlp_up(h):
        b = ag[2 + h]
        for n in range(4):
            cs = slice(n * 512, (n + 1) * 512)
            gate = dot(b, w1[:, cs])
            up = dot(b, w3[:, cs])
            hid[:, cs] = (jax.nn.silu(gate) * up).astype(BF16)

    def h1_final(h):
        y = rs_final(h)
        h1 = (x_ref[h * HP:(h + 1) * HP, :].astype(F32) + y).astype(BF16)
        h1_s[h] = h1
        ag[2 + h, rows(z), :] = norm(h1.astype(F32), gain(g2_ref))
        ag_send(2 + h)

    def out_final(h):
        y = rs_final(2 + h)
        out_ref[h * HP:(h + 1) * HP, :] = (h1_s[h].astype(F32) + y).astype(BF16)

    def table():
        p = jnp.broadcast_to(pos_ref[...].astype(F32).reshape(1, 2 * HP), (2 * HP, 2 * HP))
        r = lax.broadcasted_iota(jnp.int32, (2 * HP, 2 * HP), 0)
        k = lax.broadcasted_iota(jnp.int32, (2 * HP, 2 * HP), 1)
        p = jnp.sum(jnp.where(r == k, p, 0.0), axis=1, keepdims=True)
        ang = p * freq_ref[...]
        low = lax.broadcasted_iota(jnp.int32, (2 * HP, DH), 1) < DH // 2
        return jnp.where(low, jnp.cos(ang), jnp.sin(ang))

    sc = jax.named_scope
    with sc("start"):
        for cp in icopies:
            cp.wait()
        a = norm(x_ref[...].astype(F32), gain(g1_ref))
        for h in range(2):
            ag[h, rows(z), :] = a[h * HP:(h + 1) * HP]
        t = table()
        tab_own[...] = t
        tabg[z] = t
    with sc("bar"):
        pl.semaphore_wait(bar, 6)
    with sc("send0"):
        for d in range(1, 4):
            tab_copy(z, lax.rem(z + d, 4), d - 1).start()
            all_sends.append(lambda d=d: tab_copy(z, lax.rem(z + d, 4), d - 1))
        ag_send(0)
        ag_send(1)
    with sc("agrelay0"):
        ag_relay(0)
    with sc("agwait0"):
        ag_wait(0)
    with sc("tabwait"):
        for d in range(1, 4):
            s = lax.rem(z + d, 4)
            tab_copy(s, s, 0).wait_recv()
    with sc("wqkv"):
        for n in range(3):
            wcopies[n].wait()
    with sc("qkv0"):
        qkv(0)
    with sc("agrelay1"):
        ag_relay(1)
    with sc("kvwait0"):
        kv_wait(0)
    with sc("attn0"):
        attn(0)
    with sc("wowait"):
        wcopies[3].wait()
    with sc("rssend0"):
        rs_send(0, o_s[0], wo)
        rs_mate(0).start()
    with sc("agwait1"):
        ag_wait(1)
    with sc("qkv1"):
        qkv(1)
    with sc("rsrelay0"):
        rs_relay(0)
    with sc("kvwait1"):
        kv_wait(1)
    with sc("attn1"):
        attn(1)
    with sc("rssend1"):
        rs_send(1, o_s[1], wo)
    with sc("h1final0"):
        h1_final(0)
        rs_mate(1).start()
    with sc("rsrelay1"):
        rs_relay(1)
    with sc("agrelay2"):
        ag_relay(2)
    with sc("h1final1"):
        h1_final(1)
    with sc("agwait2"):
        ag_wait(2)
    with sc("wmlp"):
        for n in range(4, 7):
            wcopies[n].wait()
    with sc("mlp0"):
        mlp_up(0)
    with sc("rssend2"):
        rs_send(2, hid[...], w2, range(0, 2))
    with sc("agrelay3"):
        ag_relay(3)
    with sc("rssend2b"):
        rs_send(2, hid[...], w2, range(2, 3))
        rs_mate(2).start()
    with sc("agwait3"):
        ag_wait(3)
    with sc("mlp1"):
        mlp_up(1)
    with sc("rsrelay2"):
        rs_relay(2)
    with sc("rssend3"):
        rs_send(3, hid[...], w2)
        rs_mate(3).start()
    with sc("outfinal0"):
        out_final(0)
    with sc("rsrelay3"):
        rs_relay(3)
    with sc("outfinal1"):
        out_final(1)

    for s in all_sends:
        s().wait_send()

    @pl.when(outer)
    def _():
        for s in outer_sends:
            s().wait_send()

    @pl.when(inner)
    def _():
        for s in inner_sends:
            s().wait_send()


def layer(x, pos, freq, g1, g2, wq, wk, wv, wo, w1, w3, w2):
    vm = pl.BlockSpec(memory_space=pltpu.VMEM)
    hb = pl.BlockSpec(memory_space=pltpu.HBM)
    dma = pltpu.SemaphoreType.DMA
    return pl.pallas_call(
        kernel,
        out_shape=pltpu.VMEM((2 * HP, D), BF16),
        in_specs=[hb] * 12,
        out_specs=vm,
        scratch_shapes=[
            pltpu.VMEM((2 * HP, D), BF16),
            pltpu.VMEM((2 * HP,), jnp.int32),
            pltpu.VMEM((1, DH), F32),
            pltpu.VMEM((D // DH, DH), BF16),
            pltpu.VMEM((D // DH, DH), BF16),
            pltpu.VMEM((D, QC + 2 * KC), BF16),
            pltpu.VMEM((QC, D), BF16),
            pltpu.VMEM((D, FL), BF16),
            pltpu.VMEM((D, FL), BF16),
            pltpu.VMEM((FL, D), BF16),
            pltpu.VMEM((4, HR, D), BF16),
            pltpu.VMEM((2 * HP, DH), F32),
            pltpu.VMEM((4, 2 * HP, DH), F32),
            pltpu.VMEM((2, HR, QC), BF16),
            pltpu.VMEM((2, 4, HR, 2 * KC), BF16),
            pltpu.VMEM((2, HR, QC), BF16),
            pltpu.VMEM((HR, FL), BF16),
            pltpu.VMEM((2, HR, D), F32),
            pltpu.VMEM((4, HR, D), BF16),
            pltpu.VMEM((4, 2 * HP, D), BF16),
            pltpu.VMEM((4, 2, HP, D), BF16),
            pltpu.VMEM((2, HP, D), BF16),
            dma((5,)),
            dma((7,)),
            dma((4, 4)),
            dma((4, 4)),
            dma((3,)),
            dma((4,)),
            dma((2, 3)),
            dma((2, 4)),
            dma((4, NC + 1, 3)),
            dma((4, NC)),
            dma((4, 2, NC)),
        ],
        compiler_params=pltpu.CompilerParams(
            collective_id=0, has_side_effects=True, vmem_limit_bytes=58 * 2**20),
        name="layer",
    )(x, pos, freq, g1, g2, wq, wk, wv, wo, w1, w3, w2)


def solution(mesh):
    tok = P(('dp', 'cp', 'tp'), None)
    col = P(None, 'tp')
    row = P('tp', None)

    def local(x, pos, g1, g2, wq, wk, wv, wo, w1, w3, w2):
        f = 1.0 / THETA ** (np.arange(0, DH, 2) / DH)
        freq = jnp.asarray(np.concatenate([f, f])[None].astype(np.float32))
        return layer(x, pos, freq, g1.reshape(D // DH, DH), g2.reshape(D // DH, DH), wq, wk, wv, wo, w1, w3, w2)

    return jax.shard_map(local, mesh=mesh, in_specs=(tok, P(('dp', 'cp', 'tp')), P(None), P(None), col, col, col, row, col, col, row), out_specs=tok, check_vma=False)
```

```python
import math
import jax
import numpy as np
import jax.numpy as jnp
from jax import lax
from jax.experimental import pallas as pl
from jax.experimental.pallas import tpu as pltpu
from jax.sharding import PartitionSpec as P

DH = 128
EPS = 1e-5
THETA = 500000.0
D = 3072
HP = 16
HR = 64
QC = 768
KC = 256
FL = 2048
NC = 3
CW = D // NC
MESH = pl.DeviceIdType.MESH
F32 = jnp.float32
BF16 = jnp.bfloat16


def dot(a, b):
    return jnp.dot(a, b, preferred_element_type=F32)


def norm(vf, g):
    inv = lax.rsqrt(jnp.mean(vf * vf, axis=-1, keepdims=True) + EPS)
    return (vf * inv * g).astype(BF16)


def gain(ref):
    g = ref[...].astype(F32)
    return jnp.concatenate([g[n:n + 1] for n in range(D // DH)], axis=1)


def kernel(x_h, pos_h, freq_h, g1_h, g2_h, wq_h, wk_h, wv_h, wo_h, w1_h, w3_h, w2_h, out_ref,
           x_ref, pos_ref, freq_ref, g1_ref, g2_ref, wqkv, wo, w1, w3, w2, ag, tab_own, tabg, q_s, kv, o_s, hid, pbuf, sbuf, rin, fin, h1_s,
           xsem, wsem, ag_s, ag_r, tab_s, tab_r, kv_s, kv_r, rs_s, rin_r, fin_r):
    z = lax.axis_index("tp")
    c = lax.axis_index("cp")
    x = lax.axis_index("dp")

    def at_tp(d):
        return (x, d, c)

    def at_cp(d):
        return (x, z, d)

    side = z // 2
    o = 3 * side
    i = 1 + side
    ip = 2 - side
    op = 3 - 3 * side
    outer = z == o
    inner = z == i
    mate = o + i - z

    icopies = [pltpu.make_async_copy(src, dst, xsem.at[n]) for n, (src, dst) in enumerate([
        (x_h, x_ref), (g1_h, g1_ref), (pos_h, pos_ref), (freq_h, freq_ref), (g2_h, g2_ref)])]
    icopies[0].start()
    icopies[1].start()
    bar = pltpu.get_barrier_semaphore()
    for d in range(1, 4):
        pl.semaphore_signal(bar, inc=1, device_id=at_tp(lax.rem(z + d, 4)), device_id_type=MESH)
        pl.semaphore_signal(bar, inc=1, device_id=at_cp(lax.rem(c + d, 4)), device_id_type=MESH)
    for cp in icopies[2:]:
        cp.start()

    def rows(s, n=HP):
        return pl.ds(pl.multiple_of(s * HP, HP), n)

    wcopies = []
    for n, (src, dst) in enumerate([
        (wq_h, wqkv.at[:, pl.ds(0, QC)]), (wk_h, wqkv.at[:, pl.ds(QC, KC)]), (wv_h, wqkv.at[:, pl.ds(QC + KC, KC)]),
        (wo_h, wo), (w1_h, w1), (w3_h, w3), (w2_h, w2),
    ]):
        cp = pltpu.make_async_copy(src, dst, wsem.at[n])
        wcopies.append(cp)

    outer_sends = []
    inner_sends = []
    all_sends = []

    def ag_copy(ph, slot, dst, k):
        ref = ag.at[ph, rows(slot), :]
        return pltpu.make_async_remote_copy(
            src_ref=ref, dst_ref=ref, send_sem=ag_s.at[ph, k], recv_sem=ag_r.at[ph, slot],
            device_id=at_tp(dst), device_id_type=MESH)

    def ag_send(ph):
        @pl.when(outer)
        def _():
            for k, dst in enumerate((ip, i)):
                ag_copy(ph, z, dst, k).start()

        @pl.when(inner)
        def _():
            ag_copy(ph, z, o, 0).start()

        outer_sends.extend([(lambda k=k, dst=dst: ag_copy(ph, z, dst, k)) for k, dst in enumerate((ip, i))])
        inner_sends.extend([(lambda k=k, dst=dst: ag_copy(ph, z, dst, k)) for k, dst in enumerate((o, op, ip))])
        inner_sends.append(lambda: ag_copy(ph, op, o, 3))

    def ag_send_mid(ph):
        @pl.when(inner)
        def _():
            ag_copy(ph, z, op, 1).start()
            ag_copy(ph, z, ip, 2).start()

    def ag_relay(ph):
        @pl.when(inner)
        def _():
            ag_copy(ph, op, o, 3).wait_recv()
            ag_copy(ph, op, o, 3).start()

    def ag_wait(ph):
        ag_copy(ph, mate, mate, 0).wait_recv()
        ag_copy(ph, ip, ip, 0).wait_recv()

        @pl.when(outer)
        def _():
            ag_copy(ph, op, op, 0).wait_recv()

    base = rows((1 - side) * 2, 2 * HP)

    def cols(j):
        return pl.ds(j * CW, CW)

    def rs_far(ph, j):
        return pltpu.make_async_remote_copy(
            src_ref=sbuf.at[ph, base, cols(j)], dst_ref=rin.at[ph, :, cols(j)],
            send_sem=rs_s.at[ph, j, 0], recv_sem=rin_r.at[ph, j], device_id=at_tp(mate), device_id_type=MESH)

    def rs_mate(ph):
        return pltpu.make_async_remote_copy(
            src_ref=sbuf.at[ph, rows(mate), :], dst_ref=fin.at[ph, 0],
            send_sem=rs_s.at[ph, NC, 0], recv_sem=fin_r.at[ph, 0, 0], device_id=at_tp(mate), device_id_type=MESH)

    def rs_comb(ph, j, dst, k):
        return pltpu.make_async_remote_copy(
            src_ref=sbuf.at[ph, rows(dst), cols(j)], dst_ref=fin.at[ph, 1, :, cols(j)],
            send_sem=rs_s.at[ph, j, 1 + k], recv_sem=fin_r.at[ph, 1, j], device_id=at_tp(dst), device_id_type=MESH)

    def rs_send(ph, lhs, w, js=range(NC)):
        h = ph % 2
        for j in js:
            part = dot(lhs, w[:, j * CW:(j + 1) * CW])
            pbuf[h, :, j * CW:(j + 1) * CW] = part
            sbuf[ph, :, j * CW:(j + 1) * CW] = part.astype(BF16)

            @pl.when(outer)
            def _():
                rs_far(ph, j).start()

            outer_sends.append(lambda j=j: rs_far(ph, j))
            inner_sends.append(lambda j=j: rs_comb(ph, j, op, 0))
            inner_sends.append(lambda j=j: rs_comb(ph, j, ip, 1))
        all_sends.extend([lambda: rs_mate(ph)] if js[-1] == NC - 1 else [])

    def rs_relay(ph):
        h = ph % 2

        @pl.when(inner)
        def _():
            for j in range(NC):
                rs_far(ph, j).wait_recv()
                cs = slice(j * CW, (j + 1) * CW)
                sbuf[ph, base, cs] = (pbuf[h, base, cs] + rin[ph, :, cs].astype(F32)).astype(BF16)
                rs_comb(ph, j, op, 0).start()
                rs_comb(ph, j, ip, 1).start()

    def rs_final(ph):
        h = ph % 2
        rs_mate(ph).wait_recv()
        for j in range(NC):
            rs_comb(ph, j, op, 0).wait_recv()
        return pbuf[h, rows(z), :] + fin[ph, 0].astype(F32) + fin[ph, 1].astype(F32)

    def kv_copy(h, slot, dst, k):
        ref = kv.at[h, slot]
        return pltpu.make_async_remote_copy(
            src_ref=ref, dst_ref=ref, send_sem=kv_s.at[h, k], recv_sem=kv_r.at[h, slot],
            device_id=at_cp(dst), device_id_type=MESH)

    def kv_send(h):
        for d in range(1, 4):
            kv_copy(h, c, lax.rem(c + d, 4), d - 1).start()
            all_sends.append(lambda d=d: kv_copy(h, c, lax.rem(c + d, 4), d - 1))

    def kv_wait(h):
        for d in range(1, 4):
            s = lax.rem(c + d, 4)
            kv_copy(h, s, s, 0).wait_recv()

    def tab_copy(slot, dst, k):
        return pltpu.make_async_remote_copy(
            src_ref=tab_own, dst_ref=tabg.at[slot], send_sem=tab_s.at[k], recv_sem=tab_r.at[slot],
            device_id=at_tp(dst), device_id_type=MESH)

    def qkv(h):
        a = ag[h]
        t = tabg[:, h * HP:(h + 1) * HP, :].reshape(HR, DH)
        r = pltpu.roll(t, DH // 2, 1)
        low = lax.broadcasted_iota(jnp.int32, (HR, DH), 1) < DH // 2
        cos = jnp.where(low, t, r)
        sin = jnp.where(low, -r, t)

        def rope(y):
            return (y * cos + pltpu.roll(y, DH // 2, 1) * sin).astype(BF16)

        y = dot(a, wqkv[:, QC:])
        for n in range(2):
            kv[h, c, :, n * DH:(n + 1) * DH] = rope(y[:, n * DH:(n + 1) * DH])
        kv[h, c, :, KC:] = y[:, KC:].astype(BF16)
        kv_send(h)
        y = dot(a, wqkv[:, :QC])
        for n in range(6):
            q_s[h, :, n * DH:(n + 1) * DH] = rope(y[:, n * DH:(n + 1) * DH])

    scale = 1.0 / math.sqrt(DH)

    def dotT(a, b):
        return lax.dot_general(a, b, (((1,), (1,)), ((), ())), preferred_element_type=F32)

    def attn(h):
        nq = 3 * HR
        f = lax.broadcasted_iota(jnp.int32, (nq, 4 * HR), 0) & (HR - 1)
        kk = lax.broadcasted_iota(jnp.int32, (nq, 4 * HR), 1)
        if h == 0:
            seen = kk <= c * HR + f
        else:
            seq_q = (31 - 4 * c - (f >> 4)) * HP + (f & (HP - 1))
            seq_k = (31 - (kk >> 4)) * HP + (kk & (HP - 1))
            seen = seq_k <= seq_q
        for g in range(2):
            qg = jnp.concatenate([q_s[h, :, (3 * g + t) * DH:(3 * g + t + 1) * DH] for t in range(3)], axis=0)
            ks = [kv[e, :, :, g * DH:(g + 1) * DH].reshape(4 * HR, DH) for e in range(h + 1)]
            vs = [kv[e, :, :, KC + g * DH:KC + (g + 1) * DH].reshape(4 * HR, DH) for e in range(h + 1)]
            ss = [dotT(qg, k) * scale for k in ks]
            ss[h] = jnp.where(seen, ss[h], -1e30)
            m = jnp.max(ss[0], axis=-1, keepdims=True)
            for s in ss[1:]:
                m = jnp.maximum(m, jnp.max(s, axis=-1, keepdims=True))
            es = [jnp.exp(s - m) for s in ss]
            tot = jnp.sum(es[0], axis=-1, keepdims=True)
            for e in es[1:]:
                tot = tot + jnp.sum(e, axis=-1, keepdims=True)
            inv = 1.0 / tot
            acc = None
            for e, v in zip(es, vs):
                t = dot((e * inv).astype(BF16), v)
                acc = t if acc is None else acc + t
            for t in range(3):
                o_s[h, :, (3 * g + t) * DH:(3 * g + t + 1) * DH] = acc[t * HR:(t + 1) * HR].astype(BF16)

    def mlp_up(h):
        b = ag[2 + h]
        for n in range(4):
            cs = slice(n * 512, (n + 1) * 512)
            gate = dot(b, w1[:, cs])
            up = dot(b, w3[:, cs])
            hid[:, cs] = (jax.nn.silu(gate) * up).astype(BF16)

    def h1_final(h):
        y = rs_final(h)
        h1 = (x_ref[h * HP:(h + 1) * HP, :].astype(F32) + y).astype(BF16)
        h1_s[h] = h1
        ag[2 + h, rows(z), :] = norm(h1.astype(F32), gain(g2_ref))
        ag_send(2 + h)

    def out_final(h):
        y = rs_final(2 + h)
        out_ref[h * HP:(h + 1) * HP, :] = (h1_s[h].astype(F32) + y).astype(BF16)

    def table():
        p = jnp.broadcast_to(pos_ref[...].astype(F32).reshape(1, 2 * HP), (2 * HP, 2 * HP))
        r = lax.broadcasted_iota(jnp.int32, (2 * HP, 2 * HP), 0)
        k = lax.broadcasted_iota(jnp.int32, (2 * HP, 2 * HP), 1)
        p = jnp.sum(jnp.where(r == k, p, 0.0), axis=1, keepdims=True)
        ang = p * freq_ref[...]
        low = lax.broadcasted_iota(jnp.int32, (2 * HP, DH), 1) < DH // 2
        return jnp.where(low, jnp.cos(ang), jnp.sin(ang))

    sc = jax.named_scope
    with sc("start"):
        for cp in icopies:
            cp.wait()
        for cp in wcopies:
            cp.start()
        a = norm(x_ref[...].astype(F32), gain(g1_ref))
        for h in range(2):
            ag[h, rows(z), :] = a[h * HP:(h + 1) * HP]
        t = table()
        tab_own[...] = t
        tabg[z] = t
    with sc("bar"):
        pl.semaphore_wait(bar, 6)
    with sc("send0"):
        for d in range(1, 4):
            tab_copy(z, lax.rem(z + d, 4), d - 1).start()
            all_sends.append(lambda d=d: tab_copy(z, lax.rem(z + d, 4), d - 1))
        ag_send(0)
        ag_send_mid(0)
        ag_send(1)
        ag_send_mid(1)
    with sc("agrelay0"):
        ag_relay(0)
    with sc("agwait0"):
        ag_wait(0)
    with sc("tabwait"):
        for d in range(1, 4):
            s = lax.rem(z + d, 4)
            tab_copy(s, s, 0).wait_recv()
    with sc("wqkv"):
        for n in range(3):
            wcopies[n].wait()
    with sc("qkv0"):
        qkv(0)
    with sc("agrelay1"):
        ag_relay(1)
    with sc("kvwait0"):
        kv_wait(0)
    with sc("attn0"):
        attn(0)
    with sc("wowait"):
        wcopies[3].wait()
    with sc("rssend0"):
        rs_send(0, o_s[0], wo)
        rs_mate(0).start()
    with sc("agwait1"):
        ag_wait(1)
    with sc("qkv1"):
        qkv(1)
    with sc("rsrelay0"):
        rs_relay(0)
    with sc("kvwait1"):
        kv_wait(1)
    with sc("attn1"):
        attn(1)
    with sc("rssend1"):
        rs_send(1, o_s[1], wo)
        rs_mate(1).start()
    with sc("h1final0"):
        h1_final(0)
    with sc("rsrelay1"):
        rs_relay(1)
        ag_send_mid(2)
    with sc("agrelay2"):
        ag_relay(2)
    with sc("h1final1"):
        h1_final(1)
        ag_send_mid(3)
    with sc("agwait2"):
        ag_wait(2)
    with sc("wmlp"):
        for n in range(4, 7):
            wcopies[n].wait()
    with sc("mlp0"):
        mlp_up(0)
    with sc("agrelay3"):
        ag_relay(3)
    with sc("rssend2"):
        rs_send(2, hid[...], w2, range(0, 2))
    with sc("rssend2b"):
        rs_send(2, hid[...], w2, range(2, 3))
    with sc("agwait3"):
        ag_wait(3)
        rs_mate(2).start()
    with sc("mlp1"):
        mlp_up(1)
    with sc("rsrelay2"):
        rs_relay(2)
    with sc("rssend3"):
        rs_send(3, hid[...], w2)
        rs_mate(3).start()
    with sc("outfinal0"):
        out_final(0)
    with sc("rsrelay3"):
        rs_relay(3)
    with sc("outfinal1"):
        out_final(1)

    for s in all_sends:
        s().wait_send()

    @pl.when(outer)
    def _():
        for s in outer_sends:
            s().wait_send()

    @pl.when(inner)
    def _():
        for s in inner_sends:
            s().wait_send()


def layer(x, pos, freq, g1, g2, wq, wk, wv, wo, w1, w3, w2):
    vm = pl.BlockSpec(memory_space=pltpu.VMEM)
    hb = pl.BlockSpec(memory_space=pltpu.HBM)
    dma = pltpu.SemaphoreType.DMA
    return pl.pallas_call(
        kernel,
        out_shape=pltpu.VMEM((2 * HP, D), BF16),
        in_specs=[hb] * 12,
        out_specs=vm,
        scratch_shapes=[
            pltpu.VMEM((2 * HP, D), BF16),
            pltpu.VMEM((2 * HP,), jnp.int32),
            pltpu.VMEM((1, DH), F32),
            pltpu.VMEM((D // DH, DH), BF16),
            pltpu.VMEM((D // DH, DH), BF16),
            pltpu.VMEM((D, QC + 2 * KC), BF16),
            pltpu.VMEM((QC, D), BF16),
            pltpu.VMEM((D, FL), BF16),
            pltpu.VMEM((D, FL), BF16),
            pltpu.VMEM((FL, D), BF16),
            pltpu.VMEM((4, HR, D), BF16),
            pltpu.VMEM((2 * HP, DH), F32),
            pltpu.VMEM((4, 2 * HP, DH), F32),
            pltpu.VMEM((2, HR, QC), BF16),
            pltpu.VMEM((2, 4, HR, 2 * KC), BF16),
            pltpu.VMEM((2, HR, QC), BF16),
            pltpu.VMEM((HR, FL), BF16),
            pltpu.VMEM((2, HR, D), F32),
            pltpu.VMEM((4, HR, D), BF16),
            pltpu.VMEM((4, 2 * HP, D), BF16),
            pltpu.VMEM((4, 2, HP, D), BF16),
            pltpu.VMEM((2, HP, D), BF16),
            dma((5,)),
            dma((7,)),
            dma((4, 4)),
            dma((4, 4)),
            dma((3,)),
            dma((4,)),
            dma((2, 3)),
            dma((2, 4)),
            dma((4, NC + 1, 3)),
            dma((4, NC)),
            dma((4, 2, NC)),
        ],
        compiler_params=pltpu.CompilerParams(
            collective_id=0, has_side_effects=True, vmem_limit_bytes=58 * 2**20),
        name="layer",
    )(x, pos, freq, g1, g2, wq, wk, wv, wo, w1, w3, w2)


def solution(mesh):
    tok = P(('dp', 'cp', 'tp'), None)
    col = P(None, 'tp')
    row = P('tp', None)

    def local(x, pos, g1, g2, wq, wk, wv, wo, w1, w3, w2):
        f = 1.0 / THETA ** (np.arange(0, DH, 2) / DH)
        freq = jnp.asarray(np.concatenate([f, f])[None].astype(np.float32))
        return layer(x, pos, freq, g1.reshape(D // DH, DH), g2.reshape(D // DH, DH), wq, wk, wv, wo, w1, w3, w2)

    return jax.shard_map(local, mesh=mesh, in_specs=(tok, P(('dp', 'cp', 'tp')), P(None), P(None), col, col, col, row, col, col, row), out_specs=tok, check_vma=False)
```

```python
import math
import jax
import numpy as np
import jax.numpy as jnp
from jax import lax
from jax.experimental import pallas as pl
from jax.experimental.pallas import tpu as pltpu
from jax.sharding import PartitionSpec as P

DH = 128
EPS = 1e-5
THETA = 500000.0
D = 3072
HP = 16
HR = 64
QC = 768
KC = 256
FL = 2048
NC = 3
CW = D // NC
VIA = 2
MESH = pl.DeviceIdType.MESH
F32 = jnp.float32
BF16 = jnp.bfloat16


def dot(a, b):
    return jnp.dot(a, b, preferred_element_type=F32)


def norm(vf, g):
    inv = lax.rsqrt(jnp.mean(vf * vf, axis=-1, keepdims=True) + EPS)
    return (vf * inv * g).astype(BF16)


def gain(ref):
    g = ref[...].astype(F32)
    return jnp.concatenate([g[n:n + 1] for n in range(D // DH)], axis=1)


def kernel(x_h, pos_h, freq_h, g1_h, g2_h, wq_h, wk_h, wv_h, wo_h, w1_h, w3_h, w2_h, out_ref,
           x_ref, pos_ref, freq_ref, g1_ref, g2_ref, wqkv, wo, w1, w3, w2, ag, tab_own, tabg, q_s, kv, o_s, hid, pbuf, sbuf, rin, fin, h1_s,
           xsem, wsem, ag_s, ag_r, tab_s, tab_r, kv_s, kv_r, rs_s, rin_r, fin_r):
    z = lax.axis_index("tp")
    c = lax.axis_index("cp")
    x = lax.axis_index("dp")

    def at_tp(d):
        return (x, d, c)

    def at_cp(d):
        return (x, z, d)

    side = z // 2
    o = 3 * side
    i = 1 + side
    ip = 2 - side
    op = 3 - 3 * side
    outer = z == o
    inner = z == i
    mate = o + i - z

    icopies = [pltpu.make_async_copy(src, dst, xsem.at[n]) for n, (src, dst) in enumerate([
        (x_h, x_ref), (g1_h, g1_ref), (pos_h, pos_ref), (freq_h, freq_ref), (g2_h, g2_ref)])]
    icopies[0].start()
    icopies[1].start()
    bar = pltpu.get_barrier_semaphore()
    for d in range(1, 4):
        pl.semaphore_signal(bar, inc=1, device_id=at_tp(lax.rem(z + d, 4)), device_id_type=MESH)
        pl.semaphore_signal(bar, inc=1, device_id=at_cp(lax.rem(c + d, 4)), device_id_type=MESH)
    for cp in icopies[2:]:
        cp.start()

    def rows(s, n=HP):
        return pl.ds(pl.multiple_of(s * HP, HP), n)

    wcopies = []
    for n, (src, dst) in enumerate([
        (wq_h, wqkv.at[:, pl.ds(0, QC)]), (wk_h, wqkv.at[:, pl.ds(QC, KC)]), (wv_h, wqkv.at[:, pl.ds(QC + KC, KC)]),
        (wo_h, wo), (w1_h, w1), (w3_h, w3), (w2_h, w2),
    ]):
        cp = pltpu.make_async_copy(src, dst, wsem.at[n])
        wcopies.append(cp)

    outer_sends = []
    inner_sends = []
    all_sends = []

    def ag_copy(ph, slot, dst, k):
        ref = ag.at[ph, rows(slot), :]
        return pltpu.make_async_remote_copy(
            src_ref=ref, dst_ref=ref, send_sem=ag_s.at[ph, k], recv_sem=ag_r.at[ph, slot],
            device_id=at_tp(dst), device_id_type=MESH)

    def ag_send(ph):
        @pl.when(outer)
        def _():
            for k, dst in enumerate((ip, i)):
                ag_copy(ph, z, dst, k).start()

        @pl.when(inner)
        def _():
            ag_copy(ph, z, o, 0).start()

        outer_sends.extend([(lambda k=k, dst=dst: ag_copy(ph, z, dst, k)) for k, dst in enumerate((ip, i))])
        own = [(0, o), (2, ip)] + ([] if ph == VIA else [(1, op)])
        inner_sends.extend([(lambda k=k, dst=dst: ag_copy(ph, z, dst, k)) for k, dst in own])
        if ph == VIA:
            inner_sends.append(lambda: ag_copy(ph, ip, o, 1))
        inner_sends.append(lambda: ag_copy(ph, op, o, 3))

    def ag_send_mid(ph):
        @pl.when(inner)
        def _():
            if ph != VIA:
                ag_copy(ph, z, op, 1).start()
            ag_copy(ph, z, ip, 2).start()

    def ag_relay(ph):
        @pl.when(inner)
        def _():
            if ph == VIA:
                ag_copy(ph, ip, o, 1).wait_recv()
                ag_copy(ph, ip, o, 1).start()
            ag_copy(ph, op, o, 3).wait_recv()
            ag_copy(ph, op, o, 3).start()

    def ag_wait(ph):
        ag_copy(ph, mate, mate, 0).wait_recv()
        if ph != VIA:
            ag_copy(ph, ip, ip, 0).wait_recv()

        @pl.when(outer)
        def _():
            if ph == VIA:
                ag_copy(ph, ip, ip, 0).wait_recv()
            ag_copy(ph, op, op, 0).wait_recv()

    base = rows((1 - side) * 2, 2 * HP)

    def cols(j):
        return pl.ds(j * CW, CW)

    def rs_far(ph, j):
        return pltpu.make_async_remote_copy(
            src_ref=sbuf.at[ph, base, cols(j)], dst_ref=rin.at[ph, :, cols(j)],
            send_sem=rs_s.at[ph, j, 0], recv_sem=rin_r.at[ph, j], device_id=at_tp(mate), device_id_type=MESH)

    def rs_mate(ph):
        return pltpu.make_async_remote_copy(
            src_ref=sbuf.at[ph, rows(mate), :], dst_ref=fin.at[ph, 0],
            send_sem=rs_s.at[ph, NC, 0], recv_sem=fin_r.at[ph, 0, 0], device_id=at_tp(mate), device_id_type=MESH)

    def rs_comb(ph, j, dst, k):
        return pltpu.make_async_remote_copy(
            src_ref=sbuf.at[ph, rows(dst), cols(j)], dst_ref=fin.at[ph, 1, :, cols(j)],
            send_sem=rs_s.at[ph, j, 1 + k], recv_sem=fin_r.at[ph, 1, j], device_id=at_tp(dst), device_id_type=MESH)

    def rs_send(ph, lhs, w, js=range(NC)):
        h = ph % 2
        for j in js:
            part = dot(lhs, w[:, j * CW:(j + 1) * CW])
            pbuf[h, :, j * CW:(j + 1) * CW] = part
            sbuf[ph, :, j * CW:(j + 1) * CW] = part.astype(BF16)

            @pl.when(outer)
            def _():
                rs_far(ph, j).start()

            outer_sends.append(lambda j=j: rs_far(ph, j))
            inner_sends.append(lambda j=j: rs_comb(ph, j, op, 0))
            inner_sends.append(lambda j=j: rs_comb(ph, j, ip, 1))
        all_sends.extend([lambda: rs_mate(ph)] if js[-1] == NC - 1 else [])

    def rs_relay(ph):
        h = ph % 2

        @pl.when(inner)
        def _():
            for j in range(NC):
                rs_far(ph, j).wait_recv()
                cs = slice(j * CW, (j + 1) * CW)
                sbuf[ph, base, cs] = (pbuf[h, base, cs] + rin[ph, :, cs].astype(F32)).astype(BF16)
                rs_comb(ph, j, op, 0).start()
                rs_comb(ph, j, ip, 1).start()

    def rs_final(ph):
        h = ph % 2
        rs_mate(ph).wait_recv()
        for j in range(NC):
            rs_comb(ph, j, op, 0).wait_recv()
        return pbuf[h, rows(z), :] + fin[ph, 0].astype(F32) + fin[ph, 1].astype(F32)

    def kv_copy(h, slot, dst, k):
        ref = kv.at[h, slot]
        return pltpu.make_async_remote_copy(
            src_ref=ref, dst_ref=ref, send_sem=kv_s.at[h, k], recv_sem=kv_r.at[h, slot],
            device_id=at_cp(dst), device_id_type=MESH)

    def kv_send(h):
        for d in range(1, 4):
            kv_copy(h, c, lax.rem(c + d, 4), d - 1).start()
            all_sends.append(lambda d=d: kv_copy(h, c, lax.rem(c + d, 4), d - 1))

    def kv_wait(h):
        for d in range(1, 4):
            s = lax.rem(c + d, 4)
            kv_copy(h, s, s, 0).wait_recv()

    def tab_copy(slot, dst, k):
        return pltpu.make_async_remote_copy(
            src_ref=tab_own, dst_ref=tabg.at[slot], send_sem=tab_s.at[k], recv_sem=tab_r.at[slot],
            device_id=at_tp(dst), device_id_type=MESH)

    def qkv(h):
        a = ag[h]
        t = tabg[:, h * HP:(h + 1) * HP, :].reshape(HR, DH)
        r = pltpu.roll(t, DH // 2, 1)
        low = lax.broadcasted_iota(jnp.int32, (HR, DH), 1) < DH // 2
        cos = jnp.where(low, t, r)
        sin = jnp.where(low, -r, t)

        def rope(y):
            return (y * cos + pltpu.roll(y, DH // 2, 1) * sin).astype(BF16)

        y = dot(a, wqkv[:, QC:])
        for n in range(2):
            kv[h, c, :, n * DH:(n + 1) * DH] = rope(y[:, n * DH:(n + 1) * DH])
        kv[h, c, :, KC:] = y[:, KC:].astype(BF16)
        kv_send(h)
        y = dot(a, wqkv[:, :QC])
        for n in range(6):
            q_s[h, :, n * DH:(n + 1) * DH] = rope(y[:, n * DH:(n + 1) * DH])

    scale = 1.0 / math.sqrt(DH)

    def dotT(a, b):
        return lax.dot_general(a, b, (((1,), (1,)), ((), ())), preferred_element_type=F32)

    def attn(h):
        nq = 3 * HR
        f = lax.broadcasted_iota(jnp.int32, (nq, 4 * HR), 0) & (HR - 1)
        kk = lax.broadcasted_iota(jnp.int32, (nq, 4 * HR), 1)
        if h == 0:
            seen = kk <= c * HR + f
        else:
            seq_q = (31 - 4 * c - (f >> 4)) * HP + (f & (HP - 1))
            seq_k = (31 - (kk >> 4)) * HP + (kk & (HP - 1))
            seen = seq_k <= seq_q
        for g in range(2):
            qg = jnp.concatenate([q_s[h, :, (3 * g + t) * DH:(3 * g + t + 1) * DH] for t in range(3)], axis=0)
            ks = [kv[e, :, :, g * DH:(g + 1) * DH].reshape(4 * HR, DH) for e in range(h + 1)]
            vs = [kv[e, :, :, KC + g * DH:KC + (g + 1) * DH].reshape(4 * HR, DH) for e in range(h + 1)]
            ss = [dotT(qg, k) * scale for k in ks]
            ss[h] = jnp.where(seen, ss[h], -1e30)
            m = jnp.max(ss[0], axis=-1, keepdims=True)
            for s in ss[1:]:
                m = jnp.maximum(m, jnp.max(s, axis=-1, keepdims=True))
            es = [jnp.exp(s - m) for s in ss]
            tot = jnp.sum(es[0], axis=-1, keepdims=True)
            for e in es[1:]:
                tot = tot + jnp.sum(e, axis=-1, keepdims=True)
            inv = 1.0 / tot
            acc = None
            for e, v in zip(es, vs):
                t = dot((e * inv).astype(BF16), v)
                acc = t if acc is None else acc + t
            for t in range(3):
                o_s[h, :, (3 * g + t) * DH:(3 * g + t + 1) * DH] = acc[t * HR:(t + 1) * HR].astype(BF16)

    def mlp_up(h, ns=range(4)):
        b = ag[2 + h]
        for n in ns:
            cs = slice(n * 512, (n + 1) * 512)
            gate = dot(b, w1[:, cs])
            up = dot(b, w3[:, cs])
            hid[:, cs] = (jax.nn.silu(gate) * up).astype(BF16)

    def h1_final(h):
        y = rs_final(h)
        h1 = (x_ref[h * HP:(h + 1) * HP, :].astype(F32) + y).astype(BF16)
        h1_s[h] = h1
        ag[2 + h, rows(z), :] = norm(h1.astype(F32), gain(g2_ref))
        ag_send(2 + h)

    def out_final(h):
        y = rs_final(2 + h)
        out_ref[h * HP:(h + 1) * HP, :] = (h1_s[h].astype(F32) + y).astype(BF16)

    def table():
        p = jnp.broadcast_to(pos_ref[...].astype(F32).reshape(1, 2 * HP), (2 * HP, 2 * HP))
        r = lax.broadcasted_iota(jnp.int32, (2 * HP, 2 * HP), 0)
        k = lax.broadcasted_iota(jnp.int32, (2 * HP, 2 * HP), 1)
        p = jnp.sum(jnp.where(r == k, p, 0.0), axis=1, keepdims=True)
        ang = p * freq_ref[...]
        low = lax.broadcasted_iota(jnp.int32, (2 * HP, DH), 1) < DH // 2
        return jnp.where(low, jnp.cos(ang), jnp.sin(ang))

    def drain():
        for f in all_sends:
            f().wait_send()

        @pl.when(outer)
        def _():
            for f in outer_sends:
                f().wait_send()

        @pl.when(inner)
        def _():
            for f in inner_sends:
                f().wait_send()

        for fs in (all_sends, outer_sends, inner_sends):
            fs.clear()

    sc = jax.named_scope
    with sc("start"):
        for cp in icopies:
            cp.wait()
        for cp in wcopies:
            cp.start()
        a = norm(x_ref[...].astype(F32), gain(g1_ref))
        for h in range(2):
            ag[h, rows(z), :] = a[h * HP:(h + 1) * HP]
        t = table()
        tab_own[...] = t
        tabg[z] = t
    with sc("bar"):
        pl.semaphore_wait(bar, 6)
    with sc("send0"):
        for d in range(1, 4):
            tab_copy(z, lax.rem(z + d, 4), d - 1).start()
            all_sends.append(lambda d=d: tab_copy(z, lax.rem(z + d, 4), d - 1))
        ag_send(0)
        ag_send_mid(0)
        ag_send(1)
        ag_send_mid(1)
    with sc("agrelay0"):
        ag_relay(0)
    with sc("agwait0"):
        ag_wait(0)
    with sc("tabwait"):
        for d in range(1, 4):
            s = lax.rem(z + d, 4)
            tab_copy(s, s, 0).wait_recv()
    with sc("wqkv"):
        for n in range(3):
            wcopies[n].wait()
    with sc("qkv0"):
        qkv(0)
    with sc("agrelay1"):
        ag_relay(1)
    with sc("kvwait0"):
        kv_wait(0)
    with sc("attn0"):
        attn(0)
    with sc("wowait"):
        wcopies[3].wait()
    with sc("rssend0"):
        rs_send(0, o_s[0], wo)
        rs_mate(0).start()
    with sc("agwait1"):
        ag_wait(1)
    with sc("qkv1"):
        qkv(1)
    with sc("rsrelay0"):
        rs_relay(0)
    with sc("kvwait1"):
        kv_wait(1)
    with sc("attn1"):
        attn(1)
    with sc("rssend1"):
        rs_send(1, o_s[1], wo)
        rs_mate(1).start()
    with sc("h1final0"):
        h1_final(0)
    with sc("rsrelay1"):
        rs_relay(1)
        ag_send_mid(2)
    with sc("agrelay2"):
        ag_relay(2)
    with sc("h1final1"):
        h1_final(1)
        ag_send_mid(3)
    with sc("agwait2"):
        ag_wait(2)
    with sc("wmlp"):
        for n in range(4, 7):
            wcopies[n].wait()
    with sc("mlp0"):
        mlp_up(0, range(0, 2))
    with sc("agrelay3"):
        ag_relay(3)
    with sc("mlp0b"):
        mlp_up(0, range(2, 4))
    with sc("rssend2"):
        rs_send(2, hid[...], w2, range(0, 2))
    with sc("rssend2b"):
        rs_send(2, hid[...], w2, range(2, 3))
    with sc("agwait3"):
        ag_wait(3)
        rs_mate(2).start()
    with sc("mlp1"):
        mlp_up(1)
    with sc("rsrelay2"):
        rs_relay(2)
    keep = (list(all_sends), list(outer_sends), list(inner_sends))
    for fs in (all_sends, outer_sends, inner_sends):
        fs.clear()
    with sc("rssend3"):
        rs_send(3, hid[...], w2)
        rs_mate(3).start()
    with sc("outfinal0"):
        out_final(0)
    with sc("rsrelay3"):
        rs_relay(3)
    last = (list(all_sends), list(outer_sends), list(inner_sends))
    for fs, k in zip((all_sends, outer_sends, inner_sends), keep):
        fs[:] = k
    with sc("drain"):
        drain()
    for fs, k in zip((all_sends, outer_sends, inner_sends), last):
        fs[:] = k
    with sc("outfinal1"):
        out_final(1)
    drain()


def layer(x, pos, freq, g1, g2, wq, wk, wv, wo, w1, w3, w2):
    vm = pl.BlockSpec(memory_space=pltpu.VMEM)
    hb = pl.BlockSpec(memory_space=pltpu.HBM)
    dma = pltpu.SemaphoreType.DMA
    return pl.pallas_call(
        kernel,
        out_shape=pltpu.VMEM((2 * HP, D), BF16),
        in_specs=[hb] * 12,
        out_specs=vm,
        scratch_shapes=[
            pltpu.VMEM((2 * HP, D), BF16),
            pltpu.VMEM((2 * HP,), jnp.int32),
            pltpu.VMEM((1, DH), F32),
            pltpu.VMEM((D // DH, DH), BF16),
            pltpu.VMEM((D // DH, DH), BF16),
            pltpu.VMEM((D, QC + 2 * KC), BF16),
            pltpu.VMEM((QC, D), BF16),
            pltpu.VMEM((D, FL), BF16),
            pltpu.VMEM((D, FL), BF16),
            pltpu.VMEM((FL, D), BF16),
            pltpu.VMEM((4, HR, D), BF16),
            pltpu.VMEM((2 * HP, DH), F32),
            pltpu.VMEM((4, 2 * HP, DH), F32),
            pltpu.VMEM((2, HR, QC), BF16),
            pltpu.VMEM((2, 4, HR, 2 * KC), BF16),
            pltpu.VMEM((2, HR, QC), BF16),
            pltpu.VMEM((HR, FL), BF16),
            pltpu.VMEM((2, HR, D), F32),
            pltpu.VMEM((4, HR, D), BF16),
            pltpu.VMEM((4, 2 * HP, D), BF16),
            pltpu.VMEM((4, 2, HP, D), BF16),
            pltpu.VMEM((2, HP, D), BF16),
            dma((5,)),
            dma((7,)),
            dma((4, 4)),
            dma((4, 4)),
            dma((3,)),
            dma((4,)),
            dma((2, 3)),
            dma((2, 4)),
            dma((4, NC + 1, 3)),
            dma((4, NC)),
            dma((4, 2, NC)),
        ],
        compiler_params=pltpu.CompilerParams(
            collective_id=0, has_side_effects=True, vmem_limit_bytes=58 * 2**20),
        name="layer",
    )(x, pos, freq, g1, g2, wq, wk, wv, wo, w1, w3, w2)


def solution(mesh):
    tok = P(('dp', 'cp', 'tp'), None)
    col = P(None, 'tp')
    row = P('tp', None)

    def local(x, pos, g1, g2, wq, wk, wv, wo, w1, w3, w2):
        f = 1.0 / THETA ** (np.arange(0, DH, 2) / DH)
        freq = jnp.asarray(np.concatenate([f, f])[None].astype(np.float32))
        return layer(x, pos, freq, g1.reshape(D // DH, DH), g2.reshape(D // DH, DH), wq, wk, wv, wo, w1, w3, w2)

    return jax.shard_map(local, mesh=mesh, in_specs=(tok, P(('dp', 'cp', 'tp')), P(None), P(None), col, col, col, row, col, col, row), out_specs=tok, check_vma=False)
```

```python
import math
import jax
import numpy as np
import jax.numpy as jnp
from jax import lax
from jax.experimental import pallas as pl
from jax.experimental.pallas import tpu as pltpu
from jax.sharding import PartitionSpec as P

DH = 128
EPS = 1e-5
THETA = 500000.0
D = 3072
HP = 16
HR = 64
QC = 768
KC = 256
FL = 2048
NC = 3
CW = D // NC
FW = D // 2
MESH = pl.DeviceIdType.MESH
F32 = jnp.float32
BF16 = jnp.bfloat16


def dot(a, b):
    return jnp.dot(a, b, preferred_element_type=F32)


def norm(vf, g):
    inv = lax.rsqrt(jnp.mean(vf * vf, axis=-1, keepdims=True) + EPS)
    return (vf * inv * g).astype(BF16)


def gain(ref):
    g = ref[...].astype(F32)
    return jnp.concatenate([g[n:n + 1] for n in range(D // DH)], axis=1)


def kernel(x_h, pos_h, freq_h, g1_h, g2_h, wq_h, wk_h, wv_h, wo_h, w1_h, w3_h, w2_h, out_ref,
           x_ref, pos_ref, freq_ref, g1_ref, g2_ref, wqkv, wo, w1, w3, w2, ag, tab_own, tabg, q_s, kv, o_s, hid, pbuf, sbuf, rin, fin, h1_s,
           xsem, wsem, ag_s, ag_r, ag_f, tab_s, tab_r, kv_s, kv_r, rs_s, rin_r, fin_r):
    z = lax.axis_index("tp")
    c = lax.axis_index("cp")
    x = lax.axis_index("dp")

    def at_tp(d):
        return (x, d, c)

    def at_cp(d):
        return (x, z, d)

    side = z // 2
    o = 3 * side
    i = 1 + side
    ip = 2 - side
    op = 3 - 3 * side
    outer = z == o
    inner = z == i
    mate = o + i - z

    icopies = [pltpu.make_async_copy(src, dst, xsem.at[n]) for n, (src, dst) in enumerate([
        (x_h, x_ref), (g1_h, g1_ref), (pos_h, pos_ref), (freq_h, freq_ref), (g2_h, g2_ref)])]
    icopies[0].start()
    icopies[1].start()
    bar = pltpu.get_barrier_semaphore()
    for d in range(1, 4):
        pl.semaphore_signal(bar, inc=1, device_id=at_tp(lax.rem(z + d, 4)), device_id_type=MESH)
        pl.semaphore_signal(bar, inc=1, device_id=at_cp(lax.rem(c + d, 4)), device_id_type=MESH)
    for cp in icopies[2:]:
        cp.start()

    def rows(s, n=HP):
        return pl.ds(pl.multiple_of(s * HP, HP), n)

    wcopies = []
    for n, (src, dst) in enumerate([
        (wq_h, wqkv.at[:, pl.ds(0, QC)]), (wk_h, wqkv.at[:, pl.ds(QC, KC)]), (wv_h, wqkv.at[:, pl.ds(QC + KC, KC)]),
        (wo_h, wo), (w1_h, w1), (w3_h, w3), (w2_h, w2),
    ]):
        cp = pltpu.make_async_copy(src, dst, wsem.at[n])
        wcopies.append(cp)

    outer_sends = []
    inner_sends = []
    all_sends = []

    def ag_copy(ph, slot, dst, k):
        ref = ag.at[ph, rows(slot), :]
        return pltpu.make_async_remote_copy(
            src_ref=ref, dst_ref=ref, send_sem=ag_s.at[ph, k], recv_sem=ag_r.at[ph, slot],
            device_id=at_tp(dst), device_id_type=MESH)

    def ag_far(ph, slot, dst, j, k):
        ref = ag.at[ph, rows(slot), pl.ds(j * FW, FW)]
        return pltpu.make_async_remote_copy(
            src_ref=ref, dst_ref=ref, send_sem=ag_s.at[ph, k], recv_sem=ag_f.at[ph, j],
            device_id=at_tp(dst), device_id_type=MESH)

    def ag_send(ph):
        outs = [lambda: ag_far(ph, z, ip, 0, 0), lambda: ag_far(ph, z, ip, 1, 2), lambda: ag_copy(ph, z, i, 1)]

        @pl.when(outer)
        def _():
            for f in outs:
                f().start()

        @pl.when(inner)
        def _():
            ag_copy(ph, z, o, 0).start()

        outer_sends.extend(outs)
        inner_sends.extend([(lambda k=k, dst=dst: ag_copy(ph, z, dst, k)) for k, dst in enumerate((o, op, ip))])
        inner_sends.extend([(lambda j=j: ag_far(ph, op, o, j, 3 + j)) for j in range(2)])

    def ag_send_mid(ph):
        @pl.when(inner)
        def _():
            ag_copy(ph, z, op, 1).start()
            ag_copy(ph, z, ip, 2).start()

    def ag_relay(ph):
        @pl.when(inner)
        def _():
            for j in range(2):
                ag_far(ph, op, o, j, 3 + j).wait_recv()
                ag_far(ph, op, o, j, 3 + j).start()

    def ag_wait(ph):
        ag_copy(ph, mate, mate, 0).wait_recv()
        ag_copy(ph, ip, ip, 0).wait_recv()

        @pl.when(outer)
        def _():
            for j in range(2):
                ag_far(ph, op, op, j, 0).wait_recv()

    base = rows((1 - side) * 2, 2 * HP)

    def cols(j):
        return pl.ds(j * CW, CW)

    def rs_far(ph, j):
        return pltpu.make_async_remote_copy(
            src_ref=sbuf.at[ph, base, cols(j)], dst_ref=rin.at[ph, :, cols(j)],
            send_sem=rs_s.at[ph, 2 * j], recv_sem=rin_r.at[ph, j], device_id=at_tp(mate), device_id_type=MESH)

    def rs_mate(ph):
        return pltpu.make_async_remote_copy(
            src_ref=sbuf.at[ph, rows(mate), :], dst_ref=fin.at[ph, 0],
            send_sem=rs_s.at[ph, 2 * NC], recv_sem=fin_r.at[ph, NC], device_id=at_tp(mate), device_id_type=MESH)

    def rs_comb(ph, j, dst, k):
        return pltpu.make_async_remote_copy(
            src_ref=sbuf.at[ph, rows(dst), cols(j)], dst_ref=fin.at[ph, 1, :, cols(j)],
            send_sem=rs_s.at[ph, 2 * j + k], recv_sem=fin_r.at[ph, j], device_id=at_tp(dst), device_id_type=MESH)

    def rs_send(ph, lhs, w, js=range(NC)):
        h = ph % 2
        for j in js:
            part = dot(lhs, w[:, j * CW:(j + 1) * CW])
            pbuf[h, :, j * CW:(j + 1) * CW] = part
            sbuf[ph, :, j * CW:(j + 1) * CW] = part.astype(BF16)

            @pl.when(outer)
            def _():
                rs_far(ph, j).start()

            outer_sends.append(lambda j=j: rs_far(ph, j))
            inner_sends.append(lambda j=j: rs_comb(ph, j, op, 0))
            inner_sends.append(lambda j=j: rs_comb(ph, j, ip, 1))
        all_sends.extend([lambda: rs_mate(ph)] if js[-1] == NC - 1 else [])

    def rs_relay(ph):
        h = ph % 2

        @pl.when(inner)
        def _():
            for j in range(NC):
                rs_far(ph, j).wait_recv()
                cs = slice(j * CW, (j + 1) * CW)
                sbuf[ph, base, cs] = (pbuf[h, base, cs] + rin[ph, :, cs].astype(F32)).astype(BF16)
                rs_comb(ph, j, op, 0).start()
                rs_comb(ph, j, ip, 1).start()

    def rs_final(ph):
        h = ph % 2
        rs_mate(ph).wait_recv()
        for j in range(NC):
            rs_comb(ph, j, op, 0).wait_recv()
        return pbuf[h, rows(z), :] + fin[ph, 0].astype(F32) + fin[ph, 1].astype(F32)

    def kv_copy(h, slot, dst, k):
        ref = kv.at[h, slot]
        return pltpu.make_async_remote_copy(
            src_ref=ref, dst_ref=ref, send_sem=kv_s.at[h, k], recv_sem=kv_r.at[h, slot],
            device_id=at_cp(dst), device_id_type=MESH)

    def kv_send(h):
        for d in range(1, 4):
            kv_copy(h, c, lax.rem(c + d, 4), d - 1).start()
            all_sends.append(lambda d=d: kv_copy(h, c, lax.rem(c + d, 4), d - 1))

    def kv_wait(h):
        for d in range(1, 4):
            s = lax.rem(c + d, 4)
            kv_copy(h, s, s, 0).wait_recv()

    def tab_copy(slot, dst, k):
        return pltpu.make_async_remote_copy(
            src_ref=tab_own, dst_ref=tabg.at[slot], send_sem=tab_s.at[k], recv_sem=tab_r.at[slot],
            device_id=at_tp(dst), device_id_type=MESH)

    def qkv(h):
        a = ag[h]
        t = tabg[:, h * HP:(h + 1) * HP, :].reshape(HR, DH)
        r = pltpu.roll(t, DH // 2, 1)
        low = lax.broadcasted_iota(jnp.int32, (HR, DH), 1) < DH // 2
        cos = jnp.where(low, t, r)
        sin = jnp.where(low, -r, t)

        def rope(y):
            return (y * cos + pltpu.roll(y, DH // 2, 1) * sin).astype(BF16)

        y = dot(a, wqkv[:, QC:])
        for n in range(2):
            kv[h, c, :, n * DH:(n + 1) * DH] = rope(y[:, n * DH:(n + 1) * DH])
        kv[h, c, :, KC:] = y[:, KC:].astype(BF16)
        kv_send(h)
        y = dot(a, wqkv[:, :QC])
        for n in range(6):
            q_s[h, :, n * DH:(n + 1) * DH] = rope(y[:, n * DH:(n + 1) * DH])

    scale = 1.0 / math.sqrt(DH)

    def dotT(a, b):
        return lax.dot_general(a, b, (((1,), (1,)), ((), ())), preferred_element_type=F32)

    def attn(h):
        nq = 3 * HR
        f = lax.broadcasted_iota(jnp.int32, (nq, 4 * HR), 0) & (HR - 1)
        kk = lax.broadcasted_iota(jnp.int32, (nq, 4 * HR), 1)
        if h == 0:
            seen = kk <= c * HR + f
        else:
            seq_q = (31 - 4 * c - (f >> 4)) * HP + (f & (HP - 1))
            seq_k = (31 - (kk >> 4)) * HP + (kk & (HP - 1))
            seen = seq_k <= seq_q
        for g in range(2):
            qg = jnp.concatenate([q_s[h, :, (3 * g + t) * DH:(3 * g + t + 1) * DH] for t in range(3)], axis=0)
            ks = [kv[e, :, :, g * DH:(g + 1) * DH].reshape(4 * HR, DH) for e in range(h + 1)]
            vs = [kv[e, :, :, KC + g * DH:KC + (g + 1) * DH].reshape(4 * HR, DH) for e in range(h + 1)]
            ss = [dotT(qg, k) * scale for k in ks]
            ss[h] = jnp.where(seen, ss[h], -1e30)
            m = jnp.max(ss[0], axis=-1, keepdims=True)
            for s in ss[1:]:
                m = jnp.maximum(m, jnp.max(s, axis=-1, keepdims=True))
            es = [jnp.exp(s - m) for s in ss]
            tot = jnp.sum(es[0], axis=-1, keepdims=True)
            for e in es[1:]:
                tot = tot + jnp.sum(e, axis=-1, keepdims=True)
            inv = 1.0 / tot
            acc = None
            for e, v in zip(es, vs):
                t = dot((e * inv).astype(BF16), v)
                acc = t if acc is None else acc + t
            for t in range(3):
                o_s[h, :, (3 * g + t) * DH:(3 * g + t + 1) * DH] = acc[t * HR:(t + 1) * HR].astype(BF16)

    def mlp_up(h, ns=range(4)):
        b = ag[2 + h]
        for n in ns:
            cs = slice(n * 512, (n + 1) * 512)
            gate = dot(b, w1[:, cs])
            up = dot(b, w3[:, cs])
            hid[:, cs] = (jax.nn.silu(gate) * up).astype(BF16)

    def h1_final(h):
        y = rs_final(h)
        h1 = (x_ref[h * HP:(h + 1) * HP, :].astype(F32) + y).astype(BF16)
        h1_s[h] = h1
        ag[2 + h, rows(z), :] = norm(h1.astype(F32), gain(g2_ref))
        ag_send(2 + h)

    def out_final(h):
        y = rs_final(2 + h)
        out_ref[h * HP:(h + 1) * HP, :] = (h1_s[h].astype(F32) + y).astype(BF16)

    def table():
        p = jnp.broadcast_to(pos_ref[...].astype(F32).reshape(1, 2 * HP), (2 * HP, 2 * HP))
        r = lax.broadcasted_iota(jnp.int32, (2 * HP, 2 * HP), 0)
        k = lax.broadcasted_iota(jnp.int32, (2 * HP, 2 * HP), 1)
        p = jnp.sum(jnp.where(r == k, p, 0.0), axis=1, keepdims=True)
        ang = p * freq_ref[...]
        low = lax.broadcasted_iota(jnp.int32, (2 * HP, DH), 1) < DH // 2
        return jnp.where(low, jnp.cos(ang), jnp.sin(ang))

    def drain():
        for f in all_sends:
            f().wait_send()

        @pl.when(outer)
        def _():
            for f in outer_sends:
                f().wait_send()

        @pl.when(inner)
        def _():
            for f in inner_sends:
                f().wait_send()

        for fs in (all_sends, outer_sends, inner_sends):
            fs.clear()

    sc = jax.named_scope
    with sc("start"):
        for cp in icopies:
            cp.wait()
        for cp in wcopies:
            cp.start()
        a = norm(x_ref[...].astype(F32), gain(g1_ref))
        for h in range(2):
            ag[h, rows(z), :] = a[h * HP:(h + 1) * HP]
        t = table()
        tab_own[...] = t
        tabg[z] = t
    with sc("bar"):
        pl.semaphore_wait(bar, 6)
    with sc("send0"):
        for d in range(1, 4):
            tab_copy(z, lax.rem(z + d, 4), d - 1).start()
            all_sends.append(lambda d=d: tab_copy(z, lax.rem(z + d, 4), d - 1))
        ag_send(0)
        ag_send_mid(0)
        ag_send(1)
        ag_send_mid(1)
    with sc("agrelay0"):
        ag_relay(0)
    with sc("agwait0"):
        ag_wait(0)
    with sc("tabwait"):
        for d in range(1, 4):
            s = lax.rem(z + d, 4)
            tab_copy(s, s, 0).wait_recv()
    with sc("wqkv"):
        for n in range(3):
            wcopies[n].wait()
    with sc("qkv0"):
        qkv(0)
    with sc("agrelay1"):
        ag_relay(1)
    with sc("kvwait0"):
        kv_wait(0)
    with sc("attn0"):
        attn(0)
    with sc("wowait"):
        wcopies[3].wait()
    with sc("rssend0"):
        rs_send(0, o_s[0], wo)
        rs_mate(0).start()
    with sc("agwait1"):
        ag_wait(1)
    with sc("qkv1"):
        qkv(1)
    with sc("rsrelay0"):
        rs_relay(0)
    with sc("kvwait1"):
        kv_wait(1)
    with sc("attn1"):
        attn(1)
    with sc("rssend1"):
        rs_send(1, o_s[1], wo)
        rs_mate(1).start()
    with sc("h1final0"):
        h1_final(0)
    with sc("rsrelay1"):
        rs_relay(1)
        ag_send_mid(2)
    with sc("agrelay2"):
        ag_relay(2)
    with sc("h1final1"):
        h1_final(1)
        ag_send_mid(3)
    with sc("agwait2"):
        ag_wait(2)
    with sc("wmlp"):
        for n in range(4, 7):
            wcopies[n].wait()
    with sc("mlp0"):
        mlp_up(0, range(0, 2))
    with sc("agrelay3"):
        ag_relay(3)
    with sc("mlp0b"):
        mlp_up(0, range(2, 4))
    with sc("rssend2"):
        rs_send(2, hid[...], w2, range(0, 2))
    with sc("rssend2b"):
        rs_send(2, hid[...], w2, range(2, 3))
    with sc("agwait3"):
        ag_wait(3)
        rs_mate(2).start()
    with sc("mlp1"):
        mlp_up(1)
    with sc("rsrelay2"):
        rs_relay(2)
    keep = (list(all_sends), list(outer_sends), list(inner_sends))
    for fs in (all_sends, outer_sends, inner_sends):
        fs.clear()
    with sc("rssend3"):
        rs_send(3, hid[...], w2)
        rs_mate(3).start()
    with sc("outfinal0"):
        out_final(0)
    with sc("rsrelay3"):
        rs_relay(3)
    last = (list(all_sends), list(outer_sends), list(inner_sends))
    for fs, k in zip((all_sends, outer_sends, inner_sends), keep):
        fs[:] = k
    with sc("drain"):
        drain()
    for fs, k in zip((all_sends, outer_sends, inner_sends), last):
        fs[:] = k
    with sc("outfinal1"):
        out_final(1)
    drain()


def layer(x, pos, freq, g1, g2, wq, wk, wv, wo, w1, w3, w2):
    vm = pl.BlockSpec(memory_space=pltpu.VMEM)
    hb = pl.BlockSpec(memory_space=pltpu.HBM)
    dma = pltpu.SemaphoreType.DMA
    return pl.pallas_call(
        kernel,
        out_shape=pltpu.VMEM((2 * HP, D), BF16),
        in_specs=[hb] * 12,
        out_specs=vm,
        scratch_shapes=[
            pltpu.VMEM((2 * HP, D), BF16),
            pltpu.VMEM((2 * HP,), jnp.int32),
            pltpu.VMEM((1, DH), F32),
            pltpu.VMEM((D // DH, DH), BF16),
            pltpu.VMEM((D // DH, DH), BF16),
            pltpu.VMEM((D, QC + 2 * KC), BF16),
            pltpu.VMEM((QC, D), BF16),
            pltpu.VMEM((D, FL), BF16),
            pltpu.VMEM((D, FL), BF16),
            pltpu.VMEM((FL, D), BF16),
            pltpu.VMEM((4, HR, D), BF16),
            pltpu.VMEM((2 * HP, DH), F32),
            pltpu.VMEM((4, 2 * HP, DH), F32),
            pltpu.VMEM((2, HR, QC), BF16),
            pltpu.VMEM((2, 4, HR, 2 * KC), BF16),
            pltpu.VMEM((2, HR, QC), BF16),
            pltpu.VMEM((HR, FL), BF16),
            pltpu.VMEM((2, HR, D), F32),
            pltpu.VMEM((4, HR, D), BF16),
            pltpu.VMEM((4, 2 * HP, D), BF16),
            pltpu.VMEM((4, 2, HP, D), BF16),
            pltpu.VMEM((2, HP, D), BF16),
            dma((5,)),
            dma((7,)),
            dma((4, 5)),
            dma((4, 4)),
            dma((4, 2)),
            dma((3,)),
            dma((4,)),
            dma((2, 3)),
            dma((2, 4)),
            dma((4, 2 * NC + 1)),
            dma((4, NC)),
            dma((4, NC + 1)),
        ],
        compiler_params=pltpu.CompilerParams(
            collective_id=0, has_side_effects=True, vmem_limit_bytes=58 * 2**20),
        name="layer",
    )(x, pos, freq, g1, g2, wq, wk, wv, wo, w1, w3, w2)


def solution(mesh):
    tok = P(('dp', 'cp', 'tp'), None)
    col = P(None, 'tp')
    row = P('tp', None)

    def local(x, pos, g1, g2, wq, wk, wv, wo, w1, w3, w2):
        f = 1.0 / THETA ** (np.arange(0, DH, 2) / DH)
        freq = jnp.asarray(np.concatenate([f, f])[None].astype(np.float32))
        return layer(x, pos, freq, g1.reshape(D // DH, DH), g2.reshape(D // DH, DH), wq, wk, wv, wo, w1, w3, w2)

    return jax.shard_map(local, mesh=mesh, in_specs=(tok, P(('dp', 'cp', 'tp')), P(None), P(None), col, col, col, row, col, col, row), out_specs=tok, check_vma=False)
```

```python
import math
import jax
import numpy as np
import jax.numpy as jnp
from jax import lax
from jax.experimental import pallas as pl
from jax.experimental.pallas import tpu as pltpu
from jax.sharding import PartitionSpec as P

DH = 128
EPS = 1e-5
THETA = 500000.0
D = 3072
HP = 16
HR = 64
QC = 768
KC = 256
FL = 2048
NC = 3
CW = D // NC
FW = D // 2
MESH = pl.DeviceIdType.MESH
F32 = jnp.float32
BF16 = jnp.bfloat16


def dot(a, b):
    return jnp.dot(a, b, preferred_element_type=F32)


def norm(vf, g):
    inv = lax.rsqrt(jnp.mean(vf * vf, axis=-1, keepdims=True) + EPS)
    return (vf * inv * g).astype(BF16)


def gain(ref):
    g = ref[...].astype(F32)
    return jnp.concatenate([g[n:n + 1] for n in range(D // DH)], axis=1)


def kernel(x_h, pos_h, freq_h, g1_h, g2_h, wq_h, wk_h, wv_h, wo_h, w1_h, w3_h, w2_h, out_ref,
           x_ref, pos_ref, freq_ref, g1_ref, g2_ref, wqkv, wo, w1, w3, w2, ag, tab_own, tabg, q_s, kv, o_s, hid, pbuf, sbuf, rin, fin, h1_s,
           xsem, wsem, ag_s, ag_r, ag_f, tab_s, tab_r, kv_s, kv_r, rs_s, rin_r, fin_r):
    z = lax.axis_index("tp")
    c = lax.axis_index("cp")
    x = lax.axis_index("dp")

    def at_tp(d):
        return (x, d, c)

    def at_cp(d):
        return (x, z, d)

    side = z // 2
    o = 3 * side
    i = 1 + side
    ip = 2 - side
    op = 3 - 3 * side
    outer = z == o
    inner = z == i
    mate = o + i - z

    icopies = [pltpu.make_async_copy(src, dst, xsem.at[n]) for n, (src, dst) in enumerate([
        (x_h, x_ref), (g1_h, g1_ref), (pos_h, pos_ref), (freq_h, freq_ref), (g2_h, g2_ref)])]
    icopies[0].start()
    icopies[1].start()
    bar = pltpu.get_barrier_semaphore()
    for d in range(1, 4):
        pl.semaphore_signal(bar, inc=1, device_id=at_tp(lax.rem(z + d, 4)), device_id_type=MESH)
        pl.semaphore_signal(bar, inc=1, device_id=at_cp(lax.rem(c + d, 4)), device_id_type=MESH)
    for cp in icopies[2:]:
        cp.start()

    def rows(s, n=HP):
        return pl.ds(pl.multiple_of(s * HP, HP), n)

    wcopies = []
    for n, (src, dst) in enumerate([
        (wq_h, wqkv.at[:, pl.ds(0, QC)]), (wk_h, wqkv.at[:, pl.ds(QC, KC)]), (wv_h, wqkv.at[:, pl.ds(QC + KC, KC)]),
        (wo_h, wo), (w1_h, w1), (w3_h, w3), (w2_h, w2),
    ]):
        cp = pltpu.make_async_copy(src, dst, wsem.at[n])
        wcopies.append(cp)

    outer_sends = []
    inner_sends = []
    all_sends = []

    def ag_copy(ph, slot, dst, k):
        ref = ag.at[ph, rows(slot), :]
        return pltpu.make_async_remote_copy(
            src_ref=ref, dst_ref=ref, send_sem=ag_s.at[ph, k], recv_sem=ag_r.at[ph, slot],
            device_id=at_tp(dst), device_id_type=MESH)

    def ag_far(ph, slot, dst, j, k):
        ref = ag.at[ph, rows(slot), pl.ds(j * FW, FW)]
        return pltpu.make_async_remote_copy(
            src_ref=ref, dst_ref=ref, send_sem=ag_s.at[ph, k], recv_sem=ag_f.at[ph, j],
            device_id=at_tp(dst), device_id_type=MESH)

    def ag_send(ph):
        outs = [lambda: ag_far(ph, z, ip, 0, 0), lambda: ag_far(ph, z, ip, 1, 2), lambda: ag_copy(ph, z, i, 1)]

        @pl.when(outer)
        def _():
            for f in outs:
                f().start()

        @pl.when(inner)
        def _():
            ag_copy(ph, z, o, 0).start()

        outer_sends.extend(outs)
        inner_sends.extend([(lambda k=k, dst=dst: ag_copy(ph, z, dst, k)) for k, dst in enumerate((o, op, ip))])
        inner_sends.extend([(lambda j=j: ag_far(ph, op, o, j, 3 + j)) for j in range(2)])

    def ag_send_mid(ph):
        @pl.when(inner)
        def _():
            ag_copy(ph, z, op, 1).start()
            ag_copy(ph, z, ip, 2).start()

    def ag_relay(ph):
        @pl.when(inner)
        def _():
            for j in range(2):
                ag_far(ph, op, o, j, 3 + j).wait_recv()
                ag_far(ph, op, o, j, 3 + j).start()

    def ag_wait(ph):
        ag_copy(ph, mate, mate, 0).wait_recv()
        ag_copy(ph, ip, ip, 0).wait_recv()

        @pl.when(outer)
        def _():
            for j in range(2):
                ag_far(ph, op, op, j, 0).wait_recv()

    order = [(0, 0)] + [jn for j in range(1, NC) for jn in ((j, 0), (j - 1, 1))] + [(NC - 1, 1)]

    def cols(j):
        return pl.ds(j * CW, CW)

    def rs_far(ph, j, n):
        dst = (op, ip)[n]
        off = pl.multiple_of((dst - (1 - side) * 2) * HP, HP)
        return pltpu.make_async_remote_copy(
            src_ref=sbuf.at[ph, rows(dst), cols(j)], dst_ref=rin.at[ph, pl.ds(off, HP), cols(j)],
            send_sem=rs_s.at[ph, 2 * j + n], recv_sem=rin_r.at[ph, 2 * j + n], device_id=at_tp(mate), device_id_type=MESH)

    def rs_mate(ph):
        return pltpu.make_async_remote_copy(
            src_ref=sbuf.at[ph, rows(mate), :], dst_ref=fin.at[ph, 0],
            send_sem=rs_s.at[ph, 2 * NC], recv_sem=fin_r.at[ph, NC], device_id=at_tp(mate), device_id_type=MESH)

    def rs_comb(ph, j, dst, k):
        return pltpu.make_async_remote_copy(
            src_ref=sbuf.at[ph, rows(dst), cols(j)], dst_ref=fin.at[ph, 1, :, cols(j)],
            send_sem=rs_s.at[ph, 2 * j + k], recv_sem=fin_r.at[ph, j], device_id=at_tp(dst), device_id_type=MESH)

    def rs_send(ph, lhs, w, js=range(NC)):
        h = ph % 2
        for j in js:
            part = dot(lhs, w[:, j * CW:(j + 1) * CW])
            pbuf[h, :, j * CW:(j + 1) * CW] = part
            sbuf[ph, :, j * CW:(j + 1) * CW] = part.astype(BF16)

            now = order[:1] if j == 0 else order[2 * j - 1:2 * j + 1]
            now = now + order[-1:] if j == NC - 1 else now

            @pl.when(outer)
            def _():
                for jn in now:
                    rs_far(ph, *jn).start()

            outer_sends.extend([(lambda jn=jn: rs_far(ph, *jn)) for jn in now])
            inner_sends.append(lambda j=j: rs_comb(ph, j, op, 0))
            inner_sends.append(lambda j=j: rs_comb(ph, j, ip, 1))
        all_sends.extend([lambda: rs_mate(ph)] if js[-1] == NC - 1 else [])

    def rs_relay(ph):
        h = ph % 2

        @pl.when(inner)
        def _():
            for j, n in order:
                dst = (op, ip)[n]
                off = pl.ds(pl.multiple_of((dst - (1 - side) * 2) * HP, HP), HP)
                rs_far(ph, j, n).wait_recv()
                cs = slice(j * CW, (j + 1) * CW)
                sbuf[ph, rows(dst), cs] = (pbuf[h, rows(dst), cs] + rin[ph, off, cs].astype(F32)).astype(BF16)
                rs_comb(ph, j, dst, n).start()

    def rs_final(ph):
        h = ph % 2
        rs_mate(ph).wait_recv()
        for j in range(NC):
            rs_comb(ph, j, op, 0).wait_recv()
        return pbuf[h, rows(z), :] + fin[ph, 0].astype(F32) + fin[ph, 1].astype(F32)

    def kv_copy(h, slot, dst, k):
        ref = kv.at[h, slot]
        return pltpu.make_async_remote_copy(
            src_ref=ref, dst_ref=ref, send_sem=kv_s.at[h, k], recv_sem=kv_r.at[h, slot],
            device_id=at_cp(dst), device_id_type=MESH)

    def kv_send(h):
        for d in range(1, 4):
            kv_copy(h, c, lax.rem(c + d, 4), d - 1).start()
            all_sends.append(lambda d=d: kv_copy(h, c, lax.rem(c + d, 4), d - 1))

    def kv_wait(h):
        for d in range(1, 4):
            s = lax.rem(c + d, 4)
            kv_copy(h, s, s, 0).wait_recv()

    def tab_copy(slot, dst, k):
        return pltpu.make_async_remote_copy(
            src_ref=tab_own, dst_ref=tabg.at[slot], send_sem=tab_s.at[k], recv_sem=tab_r.at[slot],
            device_id=at_tp(dst), device_id_type=MESH)

    def qkv(h):
        a = ag[h]
        t = tabg[:, h * HP:(h + 1) * HP, :].reshape(HR, DH)
        r = pltpu.roll(t, DH // 2, 1)
        low = lax.broadcasted_iota(jnp.int32, (HR, DH), 1) < DH // 2
        cos = jnp.where(low, t, r)
        sin = jnp.where(low, -r, t)

        def rope(y):
            return (y * cos + pltpu.roll(y, DH // 2, 1) * sin).astype(BF16)

        y = dot(a, wqkv[:, QC:])
        for n in range(2):
            kv[h, c, :, n * DH:(n + 1) * DH] = rope(y[:, n * DH:(n + 1) * DH])
        kv[h, c, :, KC:] = y[:, KC:].astype(BF16)
        kv_send(h)
        y = dot(a, wqkv[:, :QC])
        for n in range(6):
            q_s[h, :, n * DH:(n + 1) * DH] = rope(y[:, n * DH:(n + 1) * DH])

    scale = 1.0 / math.sqrt(DH)

    def dotT(a, b):
        return lax.dot_general(a, b, (((1,), (1,)), ((), ())), preferred_element_type=F32)

    def attn(h):
        nq = 3 * HR
        f = lax.broadcasted_iota(jnp.int32, (nq, 4 * HR), 0) & (HR - 1)
        kk = lax.broadcasted_iota(jnp.int32, (nq, 4 * HR), 1)
        if h == 0:
            seen = kk <= c * HR + f
        else:
            seq_q = (31 - 4 * c - (f >> 4)) * HP + (f & (HP - 1))
            seq_k = (31 - (kk >> 4)) * HP + (kk & (HP - 1))
            seen = seq_k <= seq_q
        for g in range(2):
            qg = jnp.concatenate([q_s[h, :, (3 * g + t) * DH:(3 * g + t + 1) * DH] for t in range(3)], axis=0)
            ks = [kv[e, :, :, g * DH:(g + 1) * DH].reshape(4 * HR, DH) for e in range(h + 1)]
            vs = [kv[e, :, :, KC + g * DH:KC + (g + 1) * DH].reshape(4 * HR, DH) for e in range(h + 1)]
            ss = [dotT(qg, k) * scale for k in ks]
            ss[h] = jnp.where(seen, ss[h], -1e30)
            m = jnp.max(ss[0], axis=-1, keepdims=True)
            for s in ss[1:]:
                m = jnp.maximum(m, jnp.max(s, axis=-1, keepdims=True))
            es = [jnp.exp(s - m) for s in ss]
            tot = jnp.sum(es[0], axis=-1, keepdims=True)
            for e in es[1:]:
                tot = tot + jnp.sum(e, axis=-1, keepdims=True)
            inv = 1.0 / tot
            acc = None
            for e, v in zip(es, vs):
                t = dot((e * inv).astype(BF16), v)
                acc = t if acc is None else acc + t
            for t in range(3):
                o_s[h, :, (3 * g + t) * DH:(3 * g + t + 1) * DH] = acc[t * HR:(t + 1) * HR].astype(BF16)

    def mlp_up(h, ns=range(4)):
        b = ag[2 + h]
        for n in ns:
            cs = slice(n * 512, (n + 1) * 512)
            gate = dot(b, w1[:, cs])
            up = dot(b, w3[:, cs])
            hid[:, cs] = (jax.nn.silu(gate) * up).astype(BF16)

    def h1_final(h):
        y = rs_final(h)
        h1 = (x_ref[h * HP:(h + 1) * HP, :].astype(F32) + y).astype(BF16)
        h1_s[h] = h1
        ag[2 + h, rows(z), :] = norm(h1.astype(F32), gain(g2_ref))
        ag_send(2 + h)

    def out_final(h):
        y = rs_final(2 + h)
        out_ref[h * HP:(h + 1) * HP, :] = (h1_s[h].astype(F32) + y).astype(BF16)

    def table():
        p = jnp.broadcast_to(pos_ref[...].astype(F32).reshape(1, 2 * HP), (2 * HP, 2 * HP))
        r = lax.broadcasted_iota(jnp.int32, (2 * HP, 2 * HP), 0)
        k = lax.broadcasted_iota(jnp.int32, (2 * HP, 2 * HP), 1)
        p = jnp.sum(jnp.where(r == k, p, 0.0), axis=1, keepdims=True)
        ang = p * freq_ref[...]
        low = lax.broadcasted_iota(jnp.int32, (2 * HP, DH), 1) < DH // 2
        return jnp.where(low, jnp.cos(ang), jnp.sin(ang))

    def drain():
        for f in all_sends:
            f().wait_send()

        @pl.when(outer)
        def _():
            for f in outer_sends:
                f().wait_send()

        @pl.when(inner)
        def _():
            for f in inner_sends:
                f().wait_send()

        for fs in (all_sends, outer_sends, inner_sends):
            fs.clear()

    sc = jax.named_scope
    with sc("start"):
        for cp in icopies:
            cp.wait()
        for cp in wcopies:
            cp.start()
        a = norm(x_ref[...].astype(F32), gain(g1_ref))
        for h in range(2):
            ag[h, rows(z), :] = a[h * HP:(h + 1) * HP]
        t = table()
        tab_own[...] = t
        tabg[z] = t
    with sc("bar"):
        pl.semaphore_wait(bar, 6)
    with sc("send0"):
        for d in range(1, 4):
            tab_copy(z, lax.rem(z + d, 4), d - 1).start()
            all_sends.append(lambda d=d: tab_copy(z, lax.rem(z + d, 4), d - 1))
        ag_send(0)
        ag_send_mid(0)
        ag_send(1)
        ag_send_mid(1)
    with sc("agrelay0"):
        ag_relay(0)
    with sc("agwait0"):
        ag_wait(0)
    with sc("tabwait"):
        for d in range(1, 4):
            s = lax.rem(z + d, 4)
            tab_copy(s, s, 0).wait_recv()
    with sc("wqkv"):
        for n in range(3):
            wcopies[n].wait()
    with sc("qkv0"):
        qkv(0)
    with sc("agrelay1"):
        ag_relay(1)
    with sc("kvwait0"):
        kv_wait(0)
    with sc("attn0"):
        attn(0)
    with sc("wowait"):
        wcopies[3].wait()
    with sc("rssend0"):
        rs_send(0, o_s[0], wo)
        rs_mate(0).start()
    with sc("agwait1"):
        ag_wait(1)
    with sc("qkv1"):
        qkv(1)
    with sc("rsrelay0"):
        rs_relay(0)
    with sc("kvwait1"):
        kv_wait(1)
    with sc("attn1"):
        attn(1)
    with sc("rssend1"):
        rs_send(1, o_s[1], wo)
        rs_mate(1).start()
    with sc("h1final0"):
        h1_final(0)
    with sc("rsrelay1"):
        rs_relay(1)
        ag_send_mid(2)
    with sc("agrelay2"):
        ag_relay(2)
    with sc("h1final1"):
        h1_final(1)
        ag_send_mid(3)
    with sc("agwait2"):
        ag_wait(2)
    with sc("wmlp"):
        for n in range(4, 7):
            wcopies[n].wait()
    with sc("mlp0"):
        mlp_up(0, range(0, 1))
    with sc("agrelay3"):
        ag_relay(3)
    with sc("mlp0b"):
        mlp_up(0, range(1, 4))
    with sc("rssend2"):
        rs_send(2, hid[...], w2, range(0, 2))
    with sc("rssend2b"):
        rs_send(2, hid[...], w2, range(2, 3))
    with sc("agwait3"):
        ag_wait(3)
        rs_mate(2).start()
    with sc("mlp1"):
        mlp_up(1, range(0, 3))
    with sc("rsrelay2"):
        rs_relay(2)
    with sc("mlp1b"):
        mlp_up(1, range(3, 4))
    keep = (list(all_sends), list(outer_sends), list(inner_sends))
    for fs in (all_sends, outer_sends, inner_sends):
        fs.clear()
    with sc("rssend3"):
        rs_send(3, hid[...], w2)
        rs_mate(3).start()
    with sc("rsrelay3"):
        rs_relay(3)
    with sc("outfinal0"):
        out_final(0)
    last = (list(all_sends), list(outer_sends), list(inner_sends))
    for fs, k in zip((all_sends, outer_sends, inner_sends), keep):
        fs[:] = k
    with sc("drain"):
        drain()
    for fs, k in zip((all_sends, outer_sends, inner_sends), last):
        fs[:] = k
    with sc("outfinal1"):
        out_final(1)
    drain()


def layer(x, pos, freq, g1, g2, wq, wk, wv, wo, w1, w3, w2):
    vm = pl.BlockSpec(memory_space=pltpu.VMEM)
    hb = pl.BlockSpec(memory_space=pltpu.HBM)
    dma = pltpu.SemaphoreType.DMA
    return pl.pallas_call(
        kernel,
        out_shape=pltpu.VMEM((2 * HP, D), BF16),
        in_specs=[hb] * 12,
        out_specs=vm,
        scratch_shapes=[
            pltpu.VMEM((2 * HP, D), BF16),
            pltpu.VMEM((2 * HP,), jnp.int32),
            pltpu.VMEM((1, DH), F32),
            pltpu.VMEM((D // DH, DH), BF16),
            pltpu.VMEM((D // DH, DH), BF16),
            pltpu.VMEM((D, QC + 2 * KC), BF16),
            pltpu.VMEM((QC, D), BF16),
            pltpu.VMEM((D, FL), BF16),
            pltpu.VMEM((D, FL), BF16),
            pltpu.VMEM((FL, D), BF16),
            pltpu.VMEM((4, HR, D), BF16),
            pltpu.VMEM((2 * HP, DH), F32),
            pltpu.VMEM((4, 2 * HP, DH), F32),
            pltpu.VMEM((2, HR, QC), BF16),
            pltpu.VMEM((2, 4, HR, 2 * KC), BF16),
            pltpu.VMEM((2, HR, QC), BF16),
            pltpu.VMEM((HR, FL), BF16),
            pltpu.VMEM((2, HR, D), F32),
            pltpu.VMEM((4, HR, D), BF16),
            pltpu.VMEM((4, 2 * HP, D), BF16),
            pltpu.VMEM((4, 2, HP, D), BF16),
            pltpu.VMEM((2, HP, D), BF16),
            dma((5,)),
            dma((7,)),
            dma((4, 5)),
            dma((4, 4)),
            dma((4, 2)),
            dma((3,)),
            dma((4,)),
            dma((2, 3)),
            dma((2, 4)),
            dma((4, 2 * NC + 1)),
            dma((4, 2 * NC)),
            dma((4, NC + 1)),
        ],
        compiler_params=pltpu.CompilerParams(
            collective_id=0, has_side_effects=True, vmem_limit_bytes=58 * 2**20),
        name="layer",
    )(x, pos, freq, g1, g2, wq, wk, wv, wo, w1, w3, w2)


def solution(mesh):
    tok = P(('dp', 'cp', 'tp'), None)
    col = P(None, 'tp')
    row = P('tp', None)

    def local(x, pos, g1, g2, wq, wk, wv, wo, w1, w3, w2):
        f = 1.0 / THETA ** (np.arange(0, DH, 2) / DH)
        freq = jnp.asarray(np.concatenate([f, f])[None].astype(np.float32))
        return layer(x, pos, freq, g1.reshape(D // DH, DH), g2.reshape(D // DH, DH), wq, wk, wv, wo, w1, w3, w2)

    return jax.shard_map(local, mesh=mesh, in_specs=(tok, P(('dp', 'cp', 'tp')), P(None), P(None), col, col, col, row, col, col, row), out_specs=tok, check_vma=False)
```

```python
import math
import jax
import numpy as np
import jax.numpy as jnp
from jax import lax
from jax.experimental import pallas as pl
from jax.experimental.pallas import tpu as pltpu
from jax.sharding import PartitionSpec as P

DH = 128
EPS = 1e-5
THETA = 500000.0
D = 3072
HP = 16
HR = 64
QC = 768
KC = 256
FL = 2048
NC = 3
CW = D // NC
FW = D // 2
MESH = pl.DeviceIdType.MESH
F32 = jnp.float32
BF16 = jnp.bfloat16


def dot(a, b):
    return jnp.dot(a, b, preferred_element_type=F32)


def norm(vf, g):
    inv = lax.rsqrt(jnp.mean(vf * vf, axis=-1, keepdims=True) + EPS)
    return (vf * inv * g).astype(BF16)


def gain(ref):
    g = ref[...].astype(F32)
    return jnp.concatenate([g[n:n + 1] for n in range(D // DH)], axis=1)


def kernel(x_h, pos_h, freq_h, g1_h, g2_h, wq_h, wk_h, wv_h, wo_h, w1_h, w3_h, w2_h, out_ref,
           x_ref, pos_ref, freq_ref, g1_ref, g2_ref, wqkv, wo, w1, w3, w2, ag, tab_own, tabg, q_s, kv, o_s, hid, pbuf, sbuf, rin, fin, h1_s,
           xsem, wsem, ag_s, ag_r, ag_f, tab_s, tab_r, kv_s, kv_r, rs_s, rin_r, fin_r):
    z = lax.axis_index("tp")
    c = lax.axis_index("cp")
    x = lax.axis_index("dp")

    def at_tp(d):
        return (x, d, c)

    def at_cp(d):
        return (x, z, d)

    side = z // 2
    o = 3 * side
    i = 1 + side
    ip = 2 - side
    op = 3 - 3 * side
    outer = z == o
    inner = z == i
    mate = o + i - z

    icopies = [pltpu.make_async_copy(src, dst, xsem.at[n]) for n, (src, dst) in enumerate([
        (x_h, x_ref), (g1_h, g1_ref), (pos_h, pos_ref), (freq_h, freq_ref), (g2_h, g2_ref)])]
    icopies[0].start()
    icopies[1].start()
    bar = pltpu.get_barrier_semaphore()
    for d in range(1, 4):
        pl.semaphore_signal(bar, inc=1, device_id=at_tp(lax.rem(z + d, 4)), device_id_type=MESH)
        pl.semaphore_signal(bar, inc=1, device_id=at_cp(lax.rem(c + d, 4)), device_id_type=MESH)
    for cp in icopies[2:]:
        cp.start()

    def rows(s, n=HP):
        return pl.ds(pl.multiple_of(s * HP, HP), n)

    wcopies = []
    for n, (src, dst) in enumerate([
        (wq_h, wqkv.at[:, pl.ds(0, QC)]), (wk_h, wqkv.at[:, pl.ds(QC, KC)]), (wv_h, wqkv.at[:, pl.ds(QC + KC, KC)]),
        (wo_h, wo), (w1_h, w1), (w3_h, w3), (w2_h, w2),
    ]):
        cp = pltpu.make_async_copy(src, dst, wsem.at[n])
        wcopies.append(cp)

    outer_sends = []
    inner_sends = []
    all_sends = []

    def ag_copy(ph, slot, dst, k):
        ref = ag.at[ph, rows(slot), :]
        return pltpu.make_async_remote_copy(
            src_ref=ref, dst_ref=ref, send_sem=ag_s.at[ph, k], recv_sem=ag_r.at[ph, slot],
            device_id=at_tp(dst), device_id_type=MESH)

    def ag_far(ph, slot, dst, j, k):
        ref = ag.at[ph, rows(slot), pl.ds(j * FW, FW)]
        return pltpu.make_async_remote_copy(
            src_ref=ref, dst_ref=ref, send_sem=ag_s.at[ph, k], recv_sem=ag_f.at[ph, j],
            device_id=at_tp(dst), device_id_type=MESH)

    def ag_send(ph):
        outs = [lambda: ag_far(ph, z, ip, 0, 0), lambda: ag_far(ph, z, ip, 1, 2), lambda: ag_copy(ph, z, i, 1)]

        @pl.when(outer)
        def _():
            for f in outs:
                f().start()

        @pl.when(inner)
        def _():
            ag_copy(ph, z, o, 0).start()

        outer_sends.extend(outs)
        inner_sends.extend([(lambda k=k, dst=dst: ag_copy(ph, z, dst, k)) for k, dst in enumerate((o, op, ip))])
        inner_sends.extend([(lambda j=j: ag_far(ph, op, o, j, 3 + j)) for j in range(2)])

    def ag_send_mid(ph):
        @pl.when(inner)
        def _():
            ag_copy(ph, z, op, 1).start()
            ag_copy(ph, z, ip, 2).start()

    def ag_relay(ph):
        @pl.when(inner)
        def _():
            for j in range(2):
                ag_far(ph, op, o, j, 3 + j).wait_recv()
                ag_far(ph, op, o, j, 3 + j).start()

    def ag_wait(ph):
        ag_wait_mate(ph)
        ag_wait_rest(ph)

    def ag_wait_mate(ph):
        ag_copy(ph, mate, mate, 0).wait_recv()

    def ag_wait_rest(ph):
        ag_copy(ph, ip, ip, 0).wait_recv()

        @pl.when(outer)
        def _():
            for j in range(2):
                ag_far(ph, op, op, j, 0).wait_recv()

    order = [(0, 0)] + [jn for j in range(1, NC) for jn in ((j, 0), (j - 1, 1))] + [(NC - 1, 1)]

    def cols(j):
        return pl.ds(j * CW, CW)

    def rs_far(ph, j, n):
        dst = (op, ip)[n]
        off = pl.multiple_of((dst - (1 - side) * 2) * HP, HP)
        return pltpu.make_async_remote_copy(
            src_ref=sbuf.at[ph, rows(dst), cols(j)], dst_ref=rin.at[ph, pl.ds(off, HP), cols(j)],
            send_sem=rs_s.at[ph, 2 * j + n], recv_sem=rin_r.at[ph, 2 * j + n], device_id=at_tp(mate), device_id_type=MESH)

    def rs_mate(ph):
        return pltpu.make_async_remote_copy(
            src_ref=sbuf.at[ph, rows(mate), :], dst_ref=fin.at[ph, 0],
            send_sem=rs_s.at[ph, 2 * NC], recv_sem=fin_r.at[ph, NC], device_id=at_tp(mate), device_id_type=MESH)

    def rs_comb(ph, j, dst, k):
        return pltpu.make_async_remote_copy(
            src_ref=sbuf.at[ph, rows(dst), cols(j)], dst_ref=fin.at[ph, 1, :, cols(j)],
            send_sem=rs_s.at[ph, 2 * j + k], recv_sem=fin_r.at[ph, j], device_id=at_tp(dst), device_id_type=MESH)

    def rs_send(ph, lhs, w, js=range(NC)):
        h = ph % 2
        for j in js:
            part = dot(lhs, w[:, j * CW:(j + 1) * CW])
            pbuf[h, :, j * CW:(j + 1) * CW] = part
            sbuf[ph, :, j * CW:(j + 1) * CW] = part.astype(BF16)

            now = order[:1] if j == 0 else order[2 * j - 1:2 * j + 1]
            now = now + order[-1:] if j == NC - 1 else now

            @pl.when(outer)
            def _():
                for jn in now:
                    rs_far(ph, *jn).start()

            outer_sends.extend([(lambda jn=jn: rs_far(ph, *jn)) for jn in now])
            inner_sends.append(lambda j=j: rs_comb(ph, j, op, 0))
            inner_sends.append(lambda j=j: rs_comb(ph, j, ip, 1))
        all_sends.extend([lambda: rs_mate(ph)] if js[-1] == NC - 1 else [])

    def rs_relay(ph):
        h = ph % 2

        @pl.when(inner)
        def _():
            for j, n in order:
                dst = (op, ip)[n]
                off = pl.ds(pl.multiple_of((dst - (1 - side) * 2) * HP, HP), HP)
                rs_far(ph, j, n).wait_recv()
                cs = slice(j * CW, (j + 1) * CW)
                sbuf[ph, rows(dst), cs] = (pbuf[h, rows(dst), cs] + rin[ph, off, cs].astype(F32)).astype(BF16)
                rs_comb(ph, j, dst, n).start()

    def rs_final(ph):
        h = ph % 2
        rs_mate(ph).wait_recv()
        for j in range(NC):
            rs_comb(ph, j, op, 0).wait_recv()
        return pbuf[h, rows(z), :] + fin[ph, 0].astype(F32) + fin[ph, 1].astype(F32)

    def kv_copy(h, slot, dst, k):
        ref = kv.at[h, slot]
        return pltpu.make_async_remote_copy(
            src_ref=ref, dst_ref=ref, send_sem=kv_s.at[h, k], recv_sem=kv_r.at[h, slot],
            device_id=at_cp(dst), device_id_type=MESH)

    def kv_send(h):
        for d in range(1, 4):
            kv_copy(h, c, lax.rem(c + d, 4), d - 1).start()
            all_sends.append(lambda d=d: kv_copy(h, c, lax.rem(c + d, 4), d - 1))

    def kv_wait(h):
        for d in range(1, 4):
            s = lax.rem(c + d, 4)
            kv_copy(h, s, s, 0).wait_recv()

    def tab_copy(slot, dst, k):
        return pltpu.make_async_remote_copy(
            src_ref=tab_own, dst_ref=tabg.at[slot], send_sem=tab_s.at[k], recv_sem=tab_r.at[slot],
            device_id=at_tp(dst), device_id_type=MESH)

    def qkv(h):
        a = ag[h]
        t = tabg[:, h * HP:(h + 1) * HP, :].reshape(HR, DH)
        r = pltpu.roll(t, DH // 2, 1)
        low = lax.broadcasted_iota(jnp.int32, (HR, DH), 1) < DH // 2
        cos = jnp.where(low, t, r)
        sin = jnp.where(low, -r, t)

        def rope(y):
            return (y * cos + pltpu.roll(y, DH // 2, 1) * sin).astype(BF16)

        y = dot(a, wqkv[:, QC:])
        for n in range(2):
            kv[h, c, :, n * DH:(n + 1) * DH] = rope(y[:, n * DH:(n + 1) * DH])
        kv[h, c, :, KC:] = y[:, KC:].astype(BF16)
        kv_send(h)
        y = dot(a, wqkv[:, :QC])
        for n in range(6):
            q_s[h, :, n * DH:(n + 1) * DH] = rope(y[:, n * DH:(n + 1) * DH])

    scale = 1.0 / math.sqrt(DH)

    def dotT(a, b):
        return lax.dot_general(a, b, (((1,), (1,)), ((), ())), preferred_element_type=F32)

    def attn(h):
        nq = 3 * HR
        f = lax.broadcasted_iota(jnp.int32, (nq, 4 * HR), 0) & (HR - 1)
        kk = lax.broadcasted_iota(jnp.int32, (nq, 4 * HR), 1)
        if h == 0:
            seen = kk <= c * HR + f
        else:
            seq_q = (31 - 4 * c - (f >> 4)) * HP + (f & (HP - 1))
            seq_k = (31 - (kk >> 4)) * HP + (kk & (HP - 1))
            seen = seq_k <= seq_q
        for g in range(2):
            qg = jnp.concatenate([q_s[h, :, (3 * g + t) * DH:(3 * g + t + 1) * DH] for t in range(3)], axis=0)
            ks = [kv[e, :, :, g * DH:(g + 1) * DH].reshape(4 * HR, DH) for e in range(h + 1)]
            vs = [kv[e, :, :, KC + g * DH:KC + (g + 1) * DH].reshape(4 * HR, DH) for e in range(h + 1)]
            ss = [dotT(qg, k) * scale for k in ks]
            ss[h] = jnp.where(seen, ss[h], -1e30)
            m = jnp.max(ss[0], axis=-1, keepdims=True)
            for s in ss[1:]:
                m = jnp.maximum(m, jnp.max(s, axis=-1, keepdims=True))
            es = [jnp.exp(s - m) for s in ss]
            tot = jnp.sum(es[0], axis=-1, keepdims=True)
            for e in es[1:]:
                tot = tot + jnp.sum(e, axis=-1, keepdims=True)
            inv = 1.0 / tot
            acc = None
            for e, v in zip(es, vs):
                t = dot((e * inv).astype(BF16), v)
                acc = t if acc is None else acc + t
            for t in range(3):
                o_s[h, :, (3 * g + t) * DH:(3 * g + t + 1) * DH] = acc[t * HR:(t + 1) * HR].astype(BF16)

    def mlp_up(h, ns=range(4)):
        b = ag[2 + h]
        for n in ns:
            cs = slice(n * 512, (n + 1) * 512)
            gate = dot(b, w1[:, cs])
            up = dot(b, w3[:, cs])
            hid[:, cs] = (jax.nn.silu(gate) * up).astype(BF16)

    def h1_final(h):
        y = rs_final(h)
        h1 = (x_ref[h * HP:(h + 1) * HP, :].astype(F32) + y).astype(BF16)
        h1_s[h] = h1
        ag[2 + h, rows(z), :] = norm(h1.astype(F32), gain(g2_ref))
        ag_send(2 + h)

    def out_final(h):
        y = rs_final(2 + h)
        out_ref[h * HP:(h + 1) * HP, :] = (h1_s[h].astype(F32) + y).astype(BF16)

    def table():
        p = jnp.broadcast_to(pos_ref[...].astype(F32).reshape(1, 2 * HP), (2 * HP, 2 * HP))
        r = lax.broadcasted_iota(jnp.int32, (2 * HP, 2 * HP), 0)
        k = lax.broadcasted_iota(jnp.int32, (2 * HP, 2 * HP), 1)
        p = jnp.sum(jnp.where(r == k, p, 0.0), axis=1, keepdims=True)
        ang = p * freq_ref[...]
        low = lax.broadcasted_iota(jnp.int32, (2 * HP, DH), 1) < DH // 2
        return jnp.where(low, jnp.cos(ang), jnp.sin(ang))

    def drain():
        for f in all_sends:
            f().wait_send()

        @pl.when(outer)
        def _():
            for f in outer_sends:
                f().wait_send()

        @pl.when(inner)
        def _():
            for f in inner_sends:
                f().wait_send()

        for fs in (all_sends, outer_sends, inner_sends):
            fs.clear()

    sc = jax.named_scope
    with sc("start"):
        for cp in icopies:
            cp.wait()
        for cp in wcopies:
            cp.start()
        a = norm(x_ref[...].astype(F32), gain(g1_ref))
        for h in range(2):
            ag[h, rows(z), :] = a[h * HP:(h + 1) * HP]
        t = table()
        tab_own[...] = t
        tabg[z] = t
    with sc("bar"):
        pl.semaphore_wait(bar, 6)
    with sc("send0"):
        for d in range(1, 4):
            tab_copy(z, lax.rem(z + d, 4), d - 1).start()
            all_sends.append(lambda d=d: tab_copy(z, lax.rem(z + d, 4), d - 1))
        ag_send(0)
        ag_send_mid(0)
    with sc("agrelay0"):
        ag_relay(0)
        ag_wait_mate(0)
        ag_send(1)
        ag_send_mid(1)
    with sc("agwait0"):
        ag_wait_rest(0)
    with sc("tabwait"):
        for d in range(1, 4):
            s = lax.rem(z + d, 4)
            tab_copy(s, s, 0).wait_recv()
    with sc("wqkv"):
        for n in range(3):
            wcopies[n].wait()
    with sc("qkv0"):
        qkv(0)
    with sc("agrelay1"):
        ag_relay(1)
    with sc("kvwait0"):
        kv_wait(0)
    with sc("attn0"):
        attn(0)
    with sc("wowait"):
        wcopies[3].wait()
    with sc("rssend0"):
        rs_send(0, o_s[0], wo)
        rs_mate(0).start()
    with sc("agwait1"):
        ag_wait(1)
    with sc("qkv1"):
        qkv(1)
    with sc("rsrelay0"):
        rs_relay(0)
    with sc("kvwait1"):
        kv_wait(1)
    with sc("attn1"):
        attn(1)
    with sc("rssend1"):
        rs_send(1, o_s[1], wo)
        rs_mate(1).start()
    with sc("h1final0"):
        h1_final(0)
    with sc("rsrelay1"):
        rs_relay(1)
        ag_send_mid(2)
    with sc("agrelay2"):
        ag_relay(2)
    with sc("h1final1"):
        h1_final(1)
        ag_send_mid(3)
    with sc("agwait2"):
        ag_wait(2)
    with sc("wmlp"):
        for n in range(4, 7):
            wcopies[n].wait()
    with sc("mlp0"):
        mlp_up(0, range(0, 1))
    with sc("agrelay3"):
        ag_relay(3)
    with sc("mlp0b"):
        mlp_up(0, range(1, 4))
    with sc("rssend2"):
        rs_send(2, hid[...], w2, range(0, 2))
    with sc("rssend2b"):
        rs_send(2, hid[...], w2, range(2, 3))
    with sc("agwait3"):
        ag_wait(3)
        rs_mate(2).start()
    with sc("mlp1"):
        mlp_up(1, range(0, 3))
    with sc("rsrelay2"):
        rs_relay(2)
    with sc("mlp1b"):
        mlp_up(1, range(3, 4))
    keep = (list(all_sends), list(outer_sends), list(inner_sends))
    for fs in (all_sends, outer_sends, inner_sends):
        fs.clear()
    with sc("rssend3"):
        rs_send(3, hid[...], w2)
        rs_mate(3).start()
    with sc("rsrelay3"):
        rs_relay(3)
    with sc("outfinal0"):
        out_final(0)
    last = (list(all_sends), list(outer_sends), list(inner_sends))
    for fs, k in zip((all_sends, outer_sends, inner_sends), keep):
        fs[:] = k
    with sc("drain"):
        drain()
    for fs, k in zip((all_sends, outer_sends, inner_sends), last):
        fs[:] = k
    with sc("outfinal1"):
        out_final(1)
    drain()


def layer(x, pos, freq, g1, g2, wq, wk, wv, wo, w1, w3, w2):
    vm = pl.BlockSpec(memory_space=pltpu.VMEM)
    hb = pl.BlockSpec(memory_space=pltpu.HBM)
    dma = pltpu.SemaphoreType.DMA
    return pl.pallas_call(
        kernel,
        out_shape=pltpu.VMEM((2 * HP, D), BF16),
        in_specs=[hb] * 12,
        out_specs=vm,
        scratch_shapes=[
            pltpu.VMEM((2 * HP, D), BF16),
            pltpu.VMEM((2 * HP,), jnp.int32),
            pltpu.VMEM((1, DH), F32),
            pltpu.VMEM((D // DH, DH), BF16),
            pltpu.VMEM((D // DH, DH), BF16),
            pltpu.VMEM((D, QC + 2 * KC), BF16),
            pltpu.VMEM((QC, D), BF16),
            pltpu.VMEM((D, FL), BF16),
            pltpu.VMEM((D, FL), BF16),
            pltpu.VMEM((FL, D), BF16),
            pltpu.VMEM((4, HR, D), BF16),
            pltpu.VMEM((2 * HP, DH), F32),
            pltpu.VMEM((4, 2 * HP, DH), F32),
            pltpu.VMEM((2, HR, QC), BF16),
            pltpu.VMEM((2, 4, HR, 2 * KC), BF16),
            pltpu.VMEM((2, HR, QC), BF16),
            pltpu.VMEM((HR, FL), BF16),
            pltpu.VMEM((2, HR, D), F32),
            pltpu.VMEM((4, HR, D), BF16),
            pltpu.VMEM((4, 2 * HP, D), BF16),
            pltpu.VMEM((4, 2, HP, D), BF16),
            pltpu.VMEM((2, HP, D), BF16),
            dma((5,)),
            dma((7,)),
            dma((4, 5)),
            dma((4, 4)),
            dma((4, 2)),
            dma((3,)),
            dma((4,)),
            dma((2, 3)),
            dma((2, 4)),
            dma((4, 2 * NC + 1)),
            dma((4, 2 * NC)),
            dma((4, NC + 1)),
        ],
        compiler_params=pltpu.CompilerParams(
            collective_id=0, has_side_effects=True, vmem_limit_bytes=58 * 2**20),
        name="layer",
    )(x, pos, freq, g1, g2, wq, wk, wv, wo, w1, w3, w2)


def solution(mesh):
    tok = P(('dp', 'cp', 'tp'), None)
    col = P(None, 'tp')
    row = P('tp', None)

    def local(x, pos, g1, g2, wq, wk, wv, wo, w1, w3, w2):
        f = 1.0 / THETA ** (np.arange(0, DH, 2) / DH)
        freq = jnp.asarray(np.concatenate([f, f])[None].astype(np.float32))
        return layer(x, pos, freq, g1.reshape(D // DH, DH), g2.reshape(D // DH, DH), wq, wk, wv, wo, w1, w3, w2)

    return jax.shard_map(local, mesh=mesh, in_specs=(tok, P(('dp', 'cp', 'tp')), P(None), P(None), col, col, col, row, col, col, row), out_specs=tok, check_vma=False)
```
